128 devices in a mesh: layer: 2 (over core), px: 16 (over x, z), py: 4 (over y).
Axes of the slice: x: 4, y: 4, z: 4, core: 2. Of those that a mesh axis runs over, the one named last changes fastest.
Arguments:
- right_side: float32 [8, 2048, 4096], P('layer', 'px', 'py'), may hold values from -30 to 30
- row_conduct: float32 [8, 2048, 4096], P('layer', 'px', 'py'), may hold values from 0.5 to 2
- column_conduct: float32 [8, 2048, 4096], P('layer', 'px', 'py'), may hold values from 0.5 to 2
- via_conduct: float32 [8, 2048, 4096], P('layer', 'px', 'py'), may hold values from 0.5 to 4
- via_mask: int32 [8, 2048, 4096], P('layer', 'px', 'py'), may hold values 0 or 1
- ground_conduct: float32 [8, 2048, 4096], P('layer', 'px', 'py'), may hold values from 0.01 to 0.1
Outputs:
- solution_field: float32 [8, 2048, 4096], P('layer', 'px', 'py')
- residual: float32 [8, 2048, 4096], P('layer', 'px', 'py')
The draws below stay inside these ranges and needn't reach their ends.
All inputs are finite; a program needn't handle non-finite values. No bound on the sum of `via_mask` on one device may be relied on, other than what follows from the above.
Results may differ from the reference program's by a relative error of at most 0.0001.
Values sent between devices are 32-bit elements; how exact they have to be, the bound alone decides.
No kernel may reach another device: no remote copies, remote signals or barrier semaphores. Data moves between devices by JAX's collectives and lax.ppermute only.
A program may use at most 128 MiB of HBM per device.

```python
import math
import jax
import jax.numpy as jnp

ITERS = 2
LAYERS = 8
NX = 2048
NY = 4096


def draw_right_side(key, part):
    noise = jax.random.normal(key, (LAYERS, NX, NY), jnp.float32)
    rows = jnp.arange(NX, dtype=jnp.float32) / NX
    ramp = jnp.exp(jnp.log(3.0) * rows)[None, :, None]
    value = noise * ramp
    return jnp.clip(value, -30.0, 30.0)


def touch_ends(drawn, own_key, smallest, high):
    spot = [jax.random.randint(jax.random.fold_in(own_key, axis), (), 0, length) for axis, length in enumerate(drawn.shape)]
    longest = drawn.shape.index(max(drawn.shape))
    next_to = spot[:longest] + [(spot[longest] + 1) % drawn.shape[longest]] + spot[longest + 1:]
    return drawn.at[tuple(spot)].set(smallest).at[tuple(next_to)].set(high)


def shard_levels(key, dims, cuts, low, top_value):
    loudness = 1.0
    for dim, parts in cuts:
        heights = jax.random.uniform(jax.random.fold_in(jax.random.fold_in(key, 6), dim), (parts,), jnp.float32, low / len(cuts), top_value / len(cuts))
        loudness = loudness * jnp.repeat(jnp.exp(heights), dims[dim] // parts).reshape((-1,) + (1,) * (len(dims) - 1 - dim))
    return loudness


def setup_inputs(seed: int = 0) -> dict:
    streams_of = jax.random.split(jax.random.key(seed), 7)
    return {
        "right_side": draw_right_side(jax.random.fold_in(streams_of[6], 71), 0),
        "row_conduct": jnp.clip(jnp.exp(math.log(2.0) - 1.3862944 * jax.random.uniform(streams_of[1], (LAYERS, NX, NY), jnp.float32) ** shard_levels(streams_of[1], (LAYERS, NX, NY), ((0, 2), (1, 16), (2, 4)), -0.2, 0.2)), 0.5, 2.0),
        "column_conduct": jnp.clip(jnp.exp(math.log(2.0) - 1.3862944 * jax.random.uniform(streams_of[2], (LAYERS, NX, NY), jnp.float32) ** shard_levels(streams_of[2], (LAYERS, NX, NY), ((0, 2), (1, 16), (2, 4)), -0.2, 0.2)), 0.5, 2.0),
        "via_conduct": jnp.clip(jnp.exp(math.log(4.0) - 2.0794415 * jax.random.uniform(streams_of[3], (LAYERS, NX, NY), jnp.float32) ** shard_levels(streams_of[3], (LAYERS, NX, NY), ((0, 2), (1, 16), (2, 4)), -0.2, 0.2)), 0.5, 4.0),
        "via_mask": touch_ends((jax.random.randint(streams_of[4], (LAYERS, NX, NY), 0, 4) < 3).astype(jnp.int32), jax.random.fold_in(streams_of[4], 1), 0, 1),
        "ground_conduct": jnp.clip(jnp.exp(math.log(0.1) - 2.3025851 * jax.random.uniform(streams_of[5], (LAYERS, NX, NY), jnp.float32) ** shard_levels(streams_of[5], (LAYERS, NX, NY), ((0, 2), (1, 16), (2, 4)), -0.2, 0.2)), 0.01, 0.1),
    }


def factor_layers(diagonal, vertical, vertical_below, carried):
    gains = []
    inverses = []
    previous = carried
    for index in range(diagonal.shape[0]):
        inverse = 1.0 / (diagonal[index] - vertical_below[index] * previous)
        previous = vertical[index] * inverse
        gains.append(previous)
        inverses.append(inverse)
    return jnp.stack(gains), jnp.stack(inverses)


def forward_layers(residual, vertical_below, inverses, carried):
    values = []
    previous = carried
    for index in range(residual.shape[0]):
        previous = (residual[index] + vertical_below[index] * previous) * inverses[index]
        values.append(previous)
    return jnp.stack(values)


def back_layers(forward, gains, carried):
    count = forward.shape[0]
    values = [None] * count
    following = carried
    for index in range(count - 1, -1, -1):
        following = forward[index] + gains[index] * following
        values[index] = following
    return jnp.stack(values)


def operate(field, coeffs):
    diagonal, row_conduct, row_upper, column_conduct, column_left, vertical, vertical_below = coeffs
    padded = jnp.pad(field, 1)
    return (diagonal * field
            - row_conduct * padded[1:-1, 2:, 1:-1]
            - row_upper * padded[1:-1, :-2, 1:-1]
            - column_conduct * padded[1:-1, 1:-1, 2:]
            - column_left * padded[1:-1, 1:-1, :-2]
            - vertical * padded[2:, 1:-1, 1:-1]
            - vertical_below * padded[:-2, 1:-1, 1:-1])


def reference(right_side, row_conduct, column_conduct, via_conduct, via_mask, ground_conduct):
    level = jnp.arange(LAYERS, dtype=jnp.int32)
    keep = (level < LAYERS - 1).astype(right_side.dtype)[:, None, None]
    vertical = via_conduct * via_mask.astype(right_side.dtype) * keep
    row_upper = jnp.concatenate([jnp.zeros_like(row_conduct[:, :1, :]), row_conduct[:, :-1, :]], axis=1)
    column_left = jnp.concatenate([jnp.zeros_like(column_conduct[:, :, :1]), column_conduct[:, :, :-1]], axis=2)
    vertical_below = jnp.concatenate([jnp.zeros_like(vertical[:1]), vertical[:-1]], axis=0)
    diagonal = ground_conduct + row_conduct + row_upper + column_conduct + column_left + vertical + vertical_below
    coeffs = (diagonal, row_conduct, row_upper, column_conduct, column_left, vertical, vertical_below)
    plane = jnp.zeros_like(right_side[0])
    gains, inverses = factor_layers(diagonal, vertical, vertical_below, plane)

    def precondition(residual):
        forward = forward_layers(residual, vertical_below, inverses, plane)
        return back_layers(forward, gains, plane)

    solution_field = jnp.zeros_like(right_side)
    residual = right_side
    precond = precondition(residual)
    direction = precond
    rho = jnp.sum(residual * precond)
    for step in range(ITERS):
        image = operate(direction, coeffs)
        alpha = rho / jnp.sum(direction * image)
        solution_field = solution_field + alpha * direction
        residual = residual - alpha * image
        if step + 1 < ITERS:
            precond = precondition(residual)
            rho_next = jnp.sum(residual * precond)
            direction = precond + (rho_next / rho) * direction
            rho = rho_next
    return solution_field, residual
```

```python
import functools

import jax
import jax.numpy as jnp
from jax import lax
from jax.experimental import pallas as pl
from jax.experimental.pallas import tpu as pltpu
from jax.sharding import Mesh
from jax.sharding import PartitionSpec as P

RIGHT, ROW, COL, VIA, GROUND = range(5)
FIELDS = 5
SUB, LANE = 8, 128
PX = ("px_0", "px_1")
ALL = ("layer", "px_0", "px_1", "py")


def lanes(shape):
    return lax.broadcasted_iota(jnp.int32, shape, len(shape) - 1)


def sublanes(shape):
    return lax.broadcasted_iota(jnp.int32, shape, len(shape) - 2)


def tile(index):
    return pl.ds(pl.multiple_of(index * SUB, SUB), SUB)


def position():
    px = lax.axis_index("px_0") * lax.axis_size("px_1") + lax.axis_index("px_1")
    return (lax.axis_index("layer"), px, lax.axis_index("py"))


def spec_of(kind):
    return pl.BlockSpec(memory_space=kind)


def call(body, operands, kinds, outs, scratch=(), alias=None, flops=0, moved=0, limit=8 << 20):
    shapes = [
        pltpu.VMEM(o, jnp.float32) if isinstance(o, tuple) else o for o in outs
    ]
    operands = [
        pltpu.with_memory_space_constraint(o, pltpu.VMEM) if k == pltpu.VMEM else o
        for o, k in zip(operands, kinds)
    ]
    return pl.pallas_call(
        body,
        out_shape=shapes,
        in_specs=[spec_of(k) for k in kinds],
        out_specs=[spec_of(pltpu.VMEM if isinstance(o, tuple) else pl.ANY) for o in outs],
        scratch_shapes=list(scratch),
        input_output_aliases=alias or {},
        compiler_params=pltpu.CompilerParams(vmem_limit_bytes=limit),
        cost_estimate=pl.CostEstimate(flops=flops, bytes_accessed=moved, transcendentals=0),
    )(*operands)


def layer_of(core, k, depth):
    return jnp.where(core == 0, k, depth - 1 - k)


def link_of(core, k, depth):
    upper = depth - 1 if k == depth - 1 else depth - 2 - k
    return jnp.where(core == 0, k, upper)


def load_kernel(depth, rows, cols, *refs):
    (right, row, col, via, mask, ground, e0, e1, e2, e3, e4, msg_right, msg_left, masks, pack, sem) = refs
    core, _, _ = position()
    fields = (e0, e1, e2, e3, e4)
    copies = []
    for k in range(depth):
        at = layer_of(core, k, depth)
        link = link_of(core, k, depth)
        for index, (source, layer, target) in enumerate(
            (
                (right, at, e0),
                (row, at, e1),
                (col, at, e2),
                (via, link, e3),
                (ground, at, e4),
                (mask, link, None),
            )
        ):
            into = masks.at[k] if target is None else target.at[k, 0:rows, 0:cols]
            copies.append(pltpu.make_async_copy(source.at[layer], into, sem.at[index, k]))
    for copy in copies:
        copy.start()
    for copy in copies:
        copy.wait()
    below = jnp.where(core == 0, 1.0, 0.0).astype(jnp.float32)
    last = cols - LANE
    lane = lanes((SUB, LANE))

    def step(t, _):
        for k in range(depth):
            value = e3[k, tile(t), 0:cols] * masks[k, tile(t), :].astype(jnp.float32)
            if k == depth - 1:
                value = value * below
            e3[k, tile(t), 0:cols] = value
        to_right = jnp.zeros((SUB, LANE), jnp.float32)
        to_left = jnp.zeros((SUB, LANE), jnp.float32)
        for f in range(FIELDS):
            for k in range(depth):
                q = f * depth + k
                tail = fields[f][k, tile(t), last:cols]
                head = fields[f][k, tile(t), 0:LANE]
                if f == GROUND:
                    across = pltpu.roll(e2[k, tile(t), last:cols], 1, 1)
                    tail = tail + jnp.where(lane == LANE - 2, across, 0.0)
                shift = 4 * q + 2
                to_right = jnp.where((lane // 2) == 2 * q, pltpu.roll(tail, shift, 1), to_right)
                to_left = jnp.where((lane // 2) == 2 * q + 1, pltpu.roll(head, shift, 1), to_left)
        pack[0, tile(t), :] = to_right
        pack[1, tile(t), :] = to_left
        return 0

    lax.fori_loop(0, rows // SUB, step, 0)
    used = msg_right.shape[0]
    msg_right[...] = pack[0].T[0:used]
    msg_left[...] = pack[1].T[0:used]


def column_kernel(depth, rows, cols, places, *refs):
    e_in, (from_left, from_right) = refs[0:5], refs[5:7]
    e = refs[7:12]
    msg_down, msg_up, both = refs[12:15]
    _, _, py = position()
    used = from_left.shape[0]
    both[...] = jnp.zeros_like(both)
    both[0:used] = from_left[...] + from_right[...]
    both[...] = both[...].T
    lane = lanes((SUB, LANE))
    keep = ((lane < 2) & (py < places - 1)) | ((lane >= LANE - 2) & (py > 0))

    def step(t, _):
        value = both[tile(t), :]
        for f in range(FIELDS):
            for k in range(depth):
                q = f * depth + k
                shift = (LANE - (4 * q + 2)) % LANE
                got = pltpu.roll(value, shift, 1)
                e[f][k, tile(t), cols : cols + LANE] = jnp.where(
                    keep, got, 1.0 if f == GROUND else 0.0
                )
        return 0

    lax.fori_loop(0, rows // SUB, step, 0)
    wide = cols + LANE
    sub = sublanes((SUB, wide))
    end = rows - SUB
    down = up = None
    for f in range(FIELDS):
        for k in range(depth):
            q = f * depth + k
            i = q % 4
            tail = e[f][k, end:rows, :]
            head = e[f][k, 0:SUB, :]
            if f == GROUND:
                across = pltpu.roll(e[ROW][k, end:rows, :], 1, 0)
                tail = tail + jnp.where(sub == SUB - 2, across, 0.0)
            tail = pltpu.roll(tail, (2 * i + 2) % SUB, 0)
            head = pltpu.roll(head, (2 * i) % SUB, 0)
            if i == 0:
                down, up = tail, head
            else:
                down = jnp.where(sub // 2 == i, tail, down)
                up = jnp.where(sub // 2 == i, head, up)
            if i == 3:
                msg_down[(q // 4) * SUB : (q // 4 + 1) * SUB, :] = down
                msg_up[(q // 4) * SUB : (q // 4 + 1) * SUB, :] = up


def row_kernel(depth, rows, cols, places, *refs):
    e_in, (from_above, from_below) = refs[0:5], refs[5:7]
    e = refs[7:12]
    fwd, gain, inv, out = refs[12:16]
    core, px, _ = position()
    wide = cols + LANE
    sub = sublanes((SUB, wide))
    top = (sub >= SUB - 2) & (px > 0)
    low = (sub < 2) & (px < places - 1)
    for f in range(FIELDS):
        for k in range(depth):
            q = f * depth + k
            i = q % 4
            m = (q // 4) * SUB
            above = pltpu.roll(from_above[m : m + SUB, :], (SUB - 2 - 2 * i) % SUB, 0)
            under = pltpu.roll(from_below[m : m + SUB, :], (SUB - 2 * i) % SUB, 0)
            fill = 1.0 if f == GROUND else 0.0
            e[f][k, rows : rows + SUB, :] = jnp.where(top, above, jnp.where(low, under, fill))
    count = rows // SUB + 1
    upper = core == 1

    def step(t, _):
        before = jnp.where(t == 0, count - 1, t - 1)
        g = f = v = None
        for k in range(depth):
            row = e[ROW][k, tile(t), :]
            col = e[COL][k, tile(t), :]
            row_upper = pltpu.roll(jnp.where(sub == SUB - 1, e[ROW][k, tile(before), :], row), 1, 0)
            pivot = e[GROUND][k, tile(t), :] + row + row_upper + col + pltpu.roll(col, 1, 1)
            value = e[RIGHT][k, tile(t), :]
            if k:
                pivot = pivot + v * (1.0 - g)
                value = value + v * f
            v = e[VIA][k, tile(t), :]
            if k < depth - 1:
                inverse = 1.0 / (pivot + v)
                f = value * inverse
                g = v * inverse
                fwd[k, tile(t), :] = f
                gain[k, tile(t), :] = g
                inv[k, tile(t), :] = inverse
            else:
                inverse = 1.0 / (pivot + v)
                g = v * inverse
                inverse = jnp.where(upper, 0.0, inverse)
                fwd[k, tile(t), :] = value * inverse
                inv[k, tile(t), :] = inverse
                out[1, tile(t), :] = jnp.where(upper, pivot, v * (1.0 - g))
                g = jnp.where(upper, 1.0, g)
                gain[k, tile(t), :] = g
                out[0, tile(t), :] = g * value
        return 0

    lax.fori_loop(0, count, step, 0)


def back(depth, t, fwd, gain, middle, out):
    value = middle
    for k in range(depth - 1, -1, -1):
        value = fwd[k, tile(t), :] + gain[k, tile(t), :] * value
        out[k, tile(t), :] = value


def neighbours(k, t, count, sub, wide, field, row, col, z, flow):
    nxt = jnp.where(t == count - 1, 0, t + 1)
    r = row[k, tile(t), :]
    c = col[k, tile(t), :]
    after = field[k, tile(nxt), :]
    down = pltpu.roll(jnp.where(sub == 0, after, z), SUB - 1, 0)
    here = r * z
    up = pltpu.roll(jnp.where(sub == SUB - 1, flow, here), 1, 0)
    total = r * down + up + c * pltpu.roll(z, wide - 1, 1) + pltpu.roll(c * z, 1, 1)
    return (total, after, here)


def image_kernel(depth, rows, cols, places, *refs):
    (right, row, col, via, fwd, gain, inv, mine, theirs, z, w, fwd2, out, inv4) = refs
    _, px, py = position()
    wide = cols + LANE
    count = rows // SUB + 1
    sub = sublanes((SUB, wide))

    def first(t, _):
        ratio = 1.0 / (mine[1, tile(t), :] + theirs[1, tile(t), :])
        inv4[tile(t), :] = ratio
        back(depth, t, fwd, gain, (mine[0, tile(t), :] + theirs[0, tile(t), :]) * ratio, z)
        return 0

    lax.fori_loop(0, count, first, 0)
    lane = lanes((SUB, wide))
    beyond = (lane >= cols) & (lane < cols + LANE // 2) & (py == places[1] - 1)

    for k in range(depth):

        def second(t, carry, k=k):
            flow, here = carry
            total, after, flow = neighbours(k, t, count, sub, wide, z, row, col, here, flow)
            value = right[k, tile(t), :] - total
            outside = beyond | ((t == count - 1) & (sub < SUB // 2) & (px == places[0] - 1))
            value = jnp.where(outside, 0.0, value)
            w[k, tile(t), :] = value
            if k:
                value = value + via[k - 1, tile(t), :] * fwd2[k - 1, tile(t), :]
            fwd2[k, tile(t), :] = value * inv[k, tile(t), :]
            if k == depth - 1:
                out[tile(t), :] = gain[k, tile(t), :] * value
            return (flow, after)

        end = tile(count - 1)
        lax.fori_loop(0, count, second, (row[k, end, :] * z[k, end, :], z[k, tile(0), :]))


def dots_kernel(depth, rows, cols, *refs):
    (row, col, fwd2, gain, mine, theirs, inv4, right, z, w, y, v, sums) = refs
    wide = cols + LANE
    count = rows // SUB + 1
    sub = sublanes((SUB, wide))

    def first(t, _):
        back(depth, t, fwd2, gain, (mine[tile(t), :] + theirs[tile(t), :]) * inv4[tile(t), :], y)
        return 0

    lax.fori_loop(0, count, first, 0)
    zero = jnp.zeros((SUB, cols), jnp.float32)
    acc = (zero,) * 4
    for k in range(depth):

        def second(t, carry, k=k):
            flow, here, rho, c, e, g = carry
            total, after, flow = neighbours(k, t, count, sub, wide, y, row, col, here, flow)
            ww = w[k, tile(t), 0:cols]
            zz = z[k, tile(t), 0:cols]
            yy = here[:, 0:cols]
            vv = ww - total[:, 0:cols]
            v[k, tile(t), :] = vv
            rho = rho + right[k, tile(t), 0:cols] * zz
            return (flow, after, rho, c + zz * ww, e + ww * yy, g + yy * vv)

        end = tile(count - 1)
        carry = lax.fori_loop(
            0, count - 1, second, (row[k, end, :] * y[k, end, :], y[k, tile(0), :]) + acc
        )
        acc = carry[2:]
    lane = lanes(sums.shape)
    result = jnp.zeros(sums.shape, jnp.float32)
    for i, part in enumerate(acc):
        total = jnp.sum(jnp.sum(part, axis=0, keepdims=True), axis=1, keepdims=True)
        result = jnp.where(lane == i, total, result)
    sums[...] = result


def final_kernel(depth, rows, cols, *refs):
    (sums, right, z, w, y, v, x_out, r_out, x, r, sem) = refs
    core, _, _ = position()
    total = jnp.sum(sums[...], axis=0, keepdims=True)
    lane = lanes(total.shape)
    rho, c, e, g = (
        jnp.sum(jnp.where(lane == i, total, 0.0), axis=1, keepdims=True) for i in range(4)
    )
    alpha = rho / c
    rho1 = alpha * (alpha * e - c)
    beta = rho1 / rho
    curvature = c - 2.0 * alpha * e + alpha * alpha * g
    alpha1 = rho1 / (curvature - beta * rho1 / alpha)
    near = jnp.broadcast_to(alpha + alpha1 * (1.0 + beta), (SUB, cols))
    far = jnp.broadcast_to(alpha1 * alpha, (SUB, cols))
    copies = []
    for k in range(depth):

        def step(t, _, k=k):
            x[k, tile(t), :] = near * z[k, tile(t), 0:cols] - far * y[k, tile(t), 0:cols]
            r[k, tile(t), :] = (
                right[k, tile(t), 0:cols] - near * w[k, tile(t), 0:cols] + far * v[k, tile(t), :]
            )
            return 0

        lax.fori_loop(0, rows // SUB, step, 0)
        at = layer_of(core, k, depth)
        for index, (value, target) in enumerate(((x, x_out), (r, r_out))):
            copy = pltpu.make_async_copy(value.at[k], target.at[at], sem.at[index, k])
            copy.start()
            copies.append(copy)
    for copy in copies:
        copy.wait()


def shift(value, axis, by):
    count = lax.axis_size(axis)
    return lax.ppermute(value, axis, [(i, (i + by) % count) for i in range(count)])


def shards(right_side, row_conduct, column_conduct, via_conduct, via_mask, ground_conduct):
    depth, rows, cols = right_side.shape
    places = (lax.axis_size(PX), lax.axis_size("py"))
    devices = lax.axis_size(ALL)
    tall, wide = rows + SUB, cols + LANE
    ext = (depth, tall, wide)
    vmem, hbm = pltpu.VMEM, pl.ANY
    size = depth * tall * wide
    part = functools.partial

    strips = (FIELDS * depth * 4, LANE)
    *e, msg_right, msg_left = call(
        part(load_kernel, depth, rows, cols),
        [right_side, row_conduct, column_conduct, via_conduct, via_mask, ground_conduct],
        [hbm] * 6,
        [ext] * FIELDS + [strips] * 2,
        [
            pltpu.VMEM((depth, rows, cols), jnp.int32),
            pltpu.VMEM((2, rows, LANE), jnp.float32),
            pltpu.SemaphoreType.DMA((6, depth)),
        ],
        flops=size,
        moved=24 * size,
    )
    from_left = shift(msg_right, "py", 1)
    from_right = shift(msg_left, "py", -1)
    strips = (FIELDS * depth * 2, wide)
    *e, msg_down, msg_up = call(
        part(column_kernel, depth, rows, cols, places[1]),
        [*e, from_left, from_right],
        [vmem] * 7,
        [ext] * FIELDS + [strips] * 2,
        [pltpu.VMEM((rows, LANE), jnp.float32)],
        alias={i: i for i in range(FIELDS)},
        flops=size,
    )
    from_above = shift(msg_down, PX, 1)
    from_below = shift(msg_up, PX, -1)
    *e, fwd, gain, inv, mine = call(
        part(row_kernel, depth, rows, cols, places[0]),
        [*e, from_above, from_below],
        [vmem] * 7,
        [ext] * FIELDS + [ext] * 3 + [(2, tall, wide)],
        alias={i: i for i in range(FIELDS)},
        flops=30 * size,
    )
    right, row, col, via, _ = e
    theirs = shift(mine, "layer", 1)
    z, w, fwd2, mine2, inv4 = call(
        part(image_kernel, depth, rows, cols, places),
        [right, row, col, via, fwd, gain, inv, mine, theirs],
        [vmem] * 9,
        [ext] * 3 + [(tall, wide)] * 2,
        flops=30 * size,
    )
    theirs2 = shift(mine2, "layer", 1)
    y, v, sums = call(
        part(dots_kernel, depth, rows, cols),
        [row, col, fwd2, gain, mine2, theirs2, inv4, right, z, w],
        [vmem] * 10,
        [ext, (depth, rows, cols), (devices, LANE)],
        flops=30 * size,
    )
    sums = lax.all_to_all(sums.reshape(devices, 1, LANE), ALL, 0, 0).reshape(devices, LANE)
    block = jax.ShapeDtypeStruct((depth, rows, cols), jnp.float32)
    return call(
        part(final_kernel, depth, rows, cols),
        [sums, right, z, w, y, v],
        [vmem] * 6,
        [block] * 2,
        [
            pltpu.VMEM((depth, rows, cols), jnp.float32),
            pltpu.VMEM((depth, rows, cols), jnp.float32),
            pltpu.SemaphoreType.DMA((2, depth)),
        ],
        flops=10 * size,
    )


def solution(mesh):
    count = mesh.shape["px"]
    inner = 4 if count % 4 == 0 else 1
    split = Mesh(
        mesh.devices.reshape(mesh.shape["layer"], count // inner, inner, mesh.shape["py"]),
        ALL,
    )
    spec = P("layer", PX, "py")
    return jax.shard_map(
        lambda *a: tuple(shards(*a)),
        mesh=split,
        in_specs=(spec,) * 6,
        out_specs=(spec, spec),
        check_vma=False,
    )
```

```python
import functools

import jax
import jax.numpy as jnp
from jax import lax
from jax.experimental import pallas as pl
from jax.experimental.pallas import tpu as pltpu
from jax.sharding import Mesh
from jax.sharding import PartitionSpec as P

RIGHT, ROW, COL, VIA, GROUND = range(5)
FIELDS = 5
SUB, LANE = 8, 128
PX = ("px_0", "px_1")
ALL = ("layer", "px_0", "px_1", "py")


def lanes(shape):
    return lax.broadcasted_iota(jnp.int32, shape, len(shape) - 1)


def sublanes(shape):
    return lax.broadcasted_iota(jnp.int32, shape, len(shape) - 2)


def tile(index):
    return pl.ds(pl.multiple_of(index * SUB, SUB), SUB)


def position():
    px = lax.axis_index("px_0") * lax.axis_size("px_1") + lax.axis_index("px_1")
    return (lax.axis_index("layer"), px, lax.axis_index("py"))


def spec_of(kind):
    return pl.BlockSpec(memory_space=kind)


def call(body, operands, kinds, outs, scratch=(), alias=None, flops=0, moved=0, limit=8 << 20):
    shapes = [
        pltpu.VMEM(o, jnp.float32) if isinstance(o, tuple) else o for o in outs
    ]
    operands = [
        pltpu.with_memory_space_constraint(o, k) for o, k in zip(operands, kinds)
    ]
    return pl.pallas_call(
        body,
        out_shape=shapes,
        in_specs=[spec_of(k) for k in kinds],
        out_specs=[spec_of(pltpu.VMEM if isinstance(o, tuple) else pltpu.HBM) for o in outs],
        scratch_shapes=list(scratch),
        input_output_aliases=alias or {},
        compiler_params=pltpu.CompilerParams(vmem_limit_bytes=limit),
        cost_estimate=pl.CostEstimate(flops=flops, bytes_accessed=moved, transcendentals=0),
    )(*operands)


def layer_of(core, k, depth):
    return jnp.where(core == 0, k, depth - 1 - k)


def link_of(core, k, depth):
    upper = depth - 1 if k == depth - 1 else depth - 2 - k
    return jnp.where(core == 0, k, upper)


def copies_in(core, depth, rows, sources, targets, masks, sem, spans):
    copies = []
    for s, (low, high) in enumerate(spans):
        for k in range(depth):
            at, link = layer_of(core, k, depth), link_of(core, k, depth)
            for f, source in enumerate(sources):
                layer = link if f in (VIA, FIELDS) else at
                into = (
                    masks.at[k, :, s * (high - low) : (s + 1) * (high - low)]
                    if f == FIELDS
                    else targets[f].at[k, 0:rows, low:high]
                )
                copy = pltpu.make_async_copy(
                    source.at[layer, :, low:high], into, sem.at[s, f, k]
                )
                copy.start()
                copies.append(copy)
    return copies


def masked(core, depth, t, via, masks, low, high, start):
    for k in range(depth):
        value = via[k, tile(t), low:high] * masks[k, tile(t), start : start + high - low].astype(
            jnp.float32
        )
        if k == depth - 1:
            value = value * jnp.where(core == 0, 1.0, 0.0).astype(jnp.float32)
        via[k, tile(t), low:high] = value


def load_kernel(depth, rows, cols, *refs):
    sources, e = refs[0:6], refs[6:11]
    msg_right, msg_left, masks, pack, sem = refs[11:]
    core, _, _ = position()
    last = cols - LANE
    for copy in copies_in(core, depth, rows, sources, e, masks, sem, ((0, LANE), (last, cols))):
        copy.wait()
    lane = lanes((SUB, LANE))

    def step(t, _):
        masked(core, depth, t, e[VIA], masks, 0, LANE, 0)
        masked(core, depth, t, e[VIA], masks, last, cols, LANE)
        to_right = jnp.zeros((SUB, LANE), jnp.float32)
        to_left = jnp.zeros((SUB, LANE), jnp.float32)
        for f in range(FIELDS):
            for k in range(depth):
                q = f * depth + k
                tail = e[f][k, tile(t), last:cols]
                head = e[f][k, tile(t), 0:LANE]
                if f == GROUND:
                    across = pltpu.roll(e[COL][k, tile(t), last:cols], 1, 1)
                    tail = tail + jnp.where(lane == LANE - 2, across, 0.0)
                shift = 4 * q + 2
                to_right = jnp.where((lane // 2) == 2 * q, pltpu.roll(tail, shift, 1), to_right)
                to_left = jnp.where((lane // 2) == 2 * q + 1, pltpu.roll(head, shift, 1), to_left)
        pack[0, tile(t), :] = to_right
        pack[1, tile(t), :] = to_left
        return 0

    lax.fori_loop(0, rows // SUB, step, 0)
    used = msg_right.shape[0]
    msg_right[...] = pack[0].T[0:used]
    msg_left[...] = pack[1].T[0:used]


def middle_kernel(depth, rows, cols, *refs):
    sources, e, masks, sem = refs[0:6], refs[11:16], refs[16], refs[17]
    core, _, _ = position()
    low, high = LANE, cols - LANE
    for copy in copies_in(core, depth, rows, sources, e, masks, sem, ((low, high),)):
        copy.wait()

    def step(t, _):
        masked(core, depth, t, e[VIA], masks, low, high, 0)
        return 0

    lax.fori_loop(0, rows // SUB, step, 0)


def unpack_columns(depth, cols, keep, t, both, e):
    value = both[tile(t), :]
    for f in range(FIELDS):
        for k in range(depth):
            got = pltpu.roll(value, (LANE - (4 * (f * depth + k) + 2)) % LANE, 1)
            fill = 1.0 if f == GROUND else 0.0
            e[f][k, tile(t), cols : cols + LANE] = jnp.where(keep, got, fill)


def kept_columns(places):
    _, _, py = position()
    lane = lanes((SUB, LANE))
    return ((lane < 2) & (py < places - 1)) | ((lane >= LANE - 2) & (py > 0))


def column_kernel(depth, rows, cols, places, *refs):
    from_left, from_right = refs[5:7]
    e = refs[7:12]
    msg_down, msg_up, both = refs[12:15]
    used = from_left.shape[0]
    both[...] = jnp.zeros_like(both)
    both[0:used] = from_left[...] + from_right[...]
    both[...] = both[...].T
    keep = kept_columns(places)
    unpack_columns(depth, cols, keep, 0, both, e)
    unpack_columns(depth, cols, keep, rows // SUB - 1, both, e)
    wide = cols + LANE
    sub = sublanes((SUB, wide))
    end = rows - SUB
    down = up = None
    for f in range(FIELDS):
        for k in range(depth):
            q = f * depth + k
            i = q % 4
            tail = e[f][k, end:rows, :]
            head = e[f][k, 0:SUB, :]
            if f == GROUND:
                across = pltpu.roll(e[ROW][k, end:rows, :], 1, 0)
                tail = tail + jnp.where(sub == SUB - 2, across, 0.0)
            tail = pltpu.roll(tail, (2 * i + 2) % SUB, 0)
            head = pltpu.roll(head, (2 * i) % SUB, 0)
            if i == 0:
                down, up = tail, head
            else:
                down = jnp.where(sub // 2 == i, tail, down)
                up = jnp.where(sub // 2 == i, head, up)
            if i == 3:
                msg_down[(q // 4) * SUB : (q // 4 + 1) * SUB, :] = down
                msg_up[(q // 4) * SUB : (q // 4 + 1) * SUB, :] = up


def eliminate(depth, rows, cols, places, t, e, fwd, gain, inv, out):
    core, px, py = position()
    upper = core == 1
    count = rows // SUB + 1
    sub = sublanes((SUB, cols + LANE))
    before = jnp.where(t == 0, count - 1, t - 1)
    g = f = v = None
    for k in range(depth):
        row = e[ROW][k, tile(t), :]
        col = e[COL][k, tile(t), :]
        row_upper = pltpu.roll(jnp.where(sub == SUB - 1, e[ROW][k, tile(before), :], row), 1, 0)
        pivot = e[GROUND][k, tile(t), :] + row + row_upper + col + pltpu.roll(col, 1, 1)
        value = e[RIGHT][k, tile(t), :]
        if k:
            pivot = pivot + v * (1.0 - g)
            value = value + v * f
        v = e[VIA][k, tile(t), :]
        inverse = 1.0 / (pivot + v)
        g = v * inverse
        if k < depth - 1:
            f = value * inverse
            fwd[k, tile(t), :] = f
            gain[k, tile(t), :] = g
            inv[k, tile(t), :] = inverse
        else:
            inverse = jnp.where(upper, 0.0, inverse)
            fwd[k, tile(t), :] = value * inverse
            inv[k, tile(t), :] = inverse
            out[1, tile(t), :] = jnp.where(upper, pivot, v * (1.0 - g))
            g = jnp.where(upper, 1.0, g)
            gain[k, tile(t), :] = g
            out[0, tile(t), :] = g * value
    edge = (lanes((SUB, LANE)) == LANE - 1) & (py == places[1] - 1)
    for k in range(depth):
        part = e[COL][k, tile(t), cols - LANE : cols]
        e[COL][k, tile(t), cols - LANE : cols] = jnp.where(edge, 0.0, part)


def close_rows(depth, rows, places, e):
    _, px, _ = position()
    end = slice(rows - SUB, rows)
    for k in range(depth):
        row = e[ROW][k, end, :]
        edge = (sublanes(row.shape) == SUB - 1) & (px == places[0] - 1)
        e[ROW][k, end, :] = jnp.where(edge, 0.0, row)


def inner_kernel(depth, rows, cols, places, *refs):
    both, e, (fwd, gain, inv, out) = refs[5], refs[6:11], refs[11:15]
    keep = kept_columns(places[1])
    last = rows // SUB - 1

    def step(t, _):
        @pl.when(t < last)
        def _():
            unpack_columns(depth, cols, keep, t, both, e)

        eliminate(depth, rows, cols, places, t, e, fwd, gain, inv, out)
        return 0

    lax.fori_loop(1, last + 1, step, 0)


def outer_kernel(depth, rows, cols, places, *refs):
    from_above, from_below = refs[9:11]
    e, (fwd, gain, inv, out) = refs[11:16], refs[16:20]
    _, px, _ = position()
    sub = sublanes((SUB, cols + LANE))
    top = (sub >= SUB - 2) & (px > 0)
    low = (sub < 2) & (px < places[0] - 1)
    for f in range(FIELDS):
        for k in range(depth):
            q = f * depth + k
            i = q % 4
            m = (q // 4) * SUB
            above = pltpu.roll(from_above[m : m + SUB, :], (SUB - 2 - 2 * i) % SUB, 0)
            under = pltpu.roll(from_below[m : m + SUB, :], (SUB - 2 * i) % SUB, 0)
            fill = 1.0 if f == GROUND else 0.0
            e[f][k, rows : rows + SUB, :] = jnp.where(top, above, jnp.where(low, under, fill))

    def step(i, _):
        t = jnp.where(i == 0, 0, rows // SUB)
        eliminate(depth, rows, cols, places, t, e, fwd, gain, inv, out)
        return 0

    lax.fori_loop(0, 2, step, 0)
    close_rows(depth, rows, places, e)


def back(depth, t, fwd, gain, middle, out):
    value = middle
    for k in range(depth - 1, -1, -1):
        value = fwd[k, tile(t), :] + gain[k, tile(t), :] * value
        out[k, tile(t), :] = value


def neighbours(k, t, count, sub, field, row, col):
    nxt = jnp.where(t == count - 1, 0, t + 1)
    pre = jnp.where(t == 0, count - 1, t - 1)
    r = row[k, tile(t), :]
    c = col[k, tile(t), :]
    z = field[k, tile(t), :]
    down = pltpu.roll(jnp.where(sub == 0, field[k, tile(nxt), :], z), SUB - 1, 0)
    flow = row[k, tile(pre), :] * field[k, tile(pre), :]
    up = pltpu.roll(jnp.where(sub == SUB - 1, flow, r * z), 1, 0)
    total = r * down + up + c * pltpu.roll(z, z.shape[1] - 1, 1) + pltpu.roll(c * z, 1, 1)
    return (total, z)


def image_kernel(depth, rows, cols, *refs):
    (right, row, col, via, fwd, gain, inv, mine, theirs, z, w, fwd2, out, inv4) = refs
    count = rows // SUB + 1
    sub = sublanes((SUB, cols + LANE))

    def solve(t):
        ratio = 1.0 / (mine[1, tile(t), :] + theirs[1, tile(t), :])
        inv4[tile(t), :] = ratio
        back(depth, t, fwd, gain, (mine[0, tile(t), :] + theirs[0, tile(t), :]) * ratio, z)

    solve(count - 1)
    solve(0)

    def step(t, _):
        solve(jnp.minimum(t + 1, count - 1))
        f = None
        for k in range(depth):
            total, _ = neighbours(k, t, count, sub, z, row, col)
            value = right[k, tile(t), :] - total
            w[k, tile(t), :] = value
            if k:
                value = value + via[k - 1, tile(t), :] * f
            f = value * inv[k, tile(t), :]
            fwd2[k, tile(t), :] = f
            if k == depth - 1:
                out[tile(t), :] = gain[k, tile(t), :] * value
        return 0

    lax.fori_loop(0, count, step, 0)


def gathered(sums, parts):
    lane = lanes(sums.shape)
    result = jnp.zeros(sums.shape, jnp.float32)
    for i, part in enumerate(parts):
        total = jnp.sum(jnp.sum(part, axis=0, keepdims=True), axis=1, keepdims=True)
        result = jnp.where(lane == i, total, result)
    return result


def early_kernel(depth, rows, cols, *refs):
    (right, z, w, acc) = refs

    def step(t, carry):
        rho, c = carry
        for k in range(depth):
            zz = z[k, tile(t), 0:cols]
            rho = rho + right[k, tile(t), 0:cols] * zz
            c = c + zz * w[k, tile(t), 0:cols]
        return (rho, c)

    zero = jnp.zeros((SUB, cols), jnp.float32)
    acc[0], acc[1] = lax.fori_loop(0, rows // SUB, step, (zero, zero))


def dots_kernel(depth, rows, cols, *refs):
    (row, col, fwd2, gain, mine, theirs, inv4, w, early, y, v, sums) = refs
    count = rows // SUB + 1
    sub = sublanes((SUB, cols + LANE))

    def solve(t):
        back(depth, t, fwd2, gain, (mine[tile(t), :] + theirs[tile(t), :]) * inv4[tile(t), :], y)

    solve(count - 1)
    solve(0)

    def step(t, carry):
        e, g = carry
        solve(t + 1)
        for k in range(depth):
            total, yy = neighbours(k, t, count, sub, y, row, col)
            ww = w[k, tile(t), 0:cols]
            yy = yy[:, 0:cols]
            vv = ww - total[:, 0:cols]
            v[k, tile(t), :] = vv
            e = e + ww * yy
            g = g + yy * vv
        return (e, g)

    zero = jnp.zeros((SUB, cols), jnp.float32)
    e, g = lax.fori_loop(0, count - 1, step, (zero, zero))
    sums[...] = gathered(sums, (early[0], early[1], e, g))


def final_kernel(depth, rows, cols, *refs):
    (sums, right, z, w, y, v, x_out, r_out, x, r, sem) = refs
    core, _, _ = position()
    total = jnp.sum(sums[...], axis=0, keepdims=True)
    lane = lanes(total.shape)
    rho, c, e, g = (
        jnp.sum(jnp.where(lane == i, total, 0.0), axis=1, keepdims=True) for i in range(4)
    )
    alpha = rho / c
    rho1 = alpha * (alpha * e - c)
    beta = rho1 / rho
    curvature = c - 2.0 * alpha * e + alpha * alpha * g
    alpha1 = rho1 / (curvature - beta * rho1 / alpha)
    near = jnp.broadcast_to(alpha + alpha1 * (1.0 + beta), (SUB, cols))
    far = jnp.broadcast_to(alpha1 * alpha, (SUB, cols))
    copies = []
    for k in range(depth):

        def step(t, _, k=k):
            x[k, tile(t), :] = near * z[k, tile(t), 0:cols] - far * y[k, tile(t), 0:cols]
            r[k, tile(t), :] = (
                right[k, tile(t), 0:cols] - near * w[k, tile(t), 0:cols] + far * v[k, tile(t), :]
            )
            return 0

        lax.fori_loop(0, rows // SUB, step, 0)
        at = layer_of(core, k, depth)
        for index, (value, target) in enumerate(((x, x_out), (r, r_out))):
            copy = pltpu.make_async_copy(value.at[k], target.at[at], sem.at[index, k])
            copy.start()
            copies.append(copy)
    for copy in copies:
        copy.wait()


def shift(value, axis, by):
    count = lax.axis_size(axis)
    return lax.ppermute(value, axis, [(i, (i + by) % count) for i in range(count)])


def shards(right_side, row_conduct, column_conduct, via_conduct, via_mask, ground_conduct):
    depth, rows, cols = right_side.shape
    places = (lax.axis_size(PX), lax.axis_size("py"))
    devices = lax.axis_size(ALL)
    tall, wide = rows + SUB, cols + LANE
    ext = (depth, tall, wide)
    vmem, hbm = pltpu.VMEM, pltpu.HBM
    size = depth * tall * wide
    part = functools.partial

    inputs = [right_side, row_conduct, column_conduct, via_conduct, ground_conduct, via_mask]
    strips = (FIELDS * depth * 4, LANE)
    *e, msg_right, msg_left = call(
        part(load_kernel, depth, rows, cols),
        inputs,
        [hbm] * 6,
        [ext] * FIELDS + [strips] * 2,
        [
            pltpu.VMEM((depth, rows, 2 * LANE), jnp.int32),
            pltpu.VMEM((2, rows, LANE), jnp.float32),
            pltpu.SemaphoreType.DMA((2, 6, depth)),
        ],
        flops=size,
        moved=6 * size,
    )
    from_left = shift(msg_right, "py", 1)
    from_right = shift(msg_left, "py", -1)
    e = call(
        part(middle_kernel, depth, rows, cols),
        [*inputs, *e],
        [hbm] * 6 + [vmem] * FIELDS,
        [ext] * FIELDS,
        [
            pltpu.VMEM((depth, rows, cols - 2 * LANE), jnp.int32),
            pltpu.SemaphoreType.DMA((1, 6, depth)),
        ],
        alias={6 + i: i for i in range(FIELDS)},
        flops=10 * size,
        moved=18 * size,
    )
    strips = (FIELDS * depth * 2, wide)
    *e, msg_down, msg_up, both = call(
        part(column_kernel, depth, rows, cols, places[1]),
        [*e, from_left, from_right],
        [vmem] * 7,
        [ext] * FIELDS + [strips] * 2 + [(rows, LANE)],
        alias={i: i for i in range(FIELDS)},
        flops=size,
    )
    from_above = shift(msg_down, PX, 1)
    from_below = shift(msg_up, PX, -1)
    state = call(
        part(inner_kernel, depth, rows, cols, places),
        [*e, both],
        [vmem] * 6,
        [ext] * FIELDS + [ext] * 3 + [(2, tall, wide)],
        alias={i: i for i in range(FIELDS)},
        flops=30 * size,
    )
    *e, fwd, gain, inv, mine = call(
        part(outer_kernel, depth, rows, cols, places),
        [*state, from_above, from_below],
        [vmem] * 11,
        [ext] * FIELDS + [ext] * 3 + [(2, tall, wide)],
        alias={i: i for i in range(FIELDS + 4)},
        flops=3 * size,
    )
    right, row, col, via, _ = e
    theirs = shift(mine, "layer", 1)
    z, w, fwd2, mine2, inv4 = call(
        part(image_kernel, depth, rows, cols),
        [right, row, col, via, fwd, gain, inv, mine, theirs],
        [vmem] * 9,
        [ext] * 3 + [(tall, wide)] * 2,
        flops=30 * size,
    )
    theirs2 = shift(mine2, "layer", 1)
    (early,) = call(
        part(early_kernel, depth, rows, cols),
        [right, z, w],
        [vmem] * 3,
        [(2, SUB, cols)],
        flops=4 * size,
    )
    y, v, sums = call(
        part(dots_kernel, depth, rows, cols),
        [row, col, fwd2, gain, mine2, theirs2, inv4, w, early],
        [vmem] * 9,
        [ext, (depth, rows, cols), (devices, LANE)],
        flops=30 * size,
    )
    sums = lax.all_to_all(sums.reshape(devices, 1, LANE), ALL, 0, 0).reshape(devices, LANE)
    block = jax.ShapeDtypeStruct((depth, rows, cols), jnp.float32)
    return call(
        part(final_kernel, depth, rows, cols),
        [sums, right, z, w, y, v],
        [vmem] * 6,
        [block] * 2,
        [
            pltpu.VMEM((depth, rows, cols), jnp.float32),
            pltpu.VMEM((depth, rows, cols), jnp.float32),
            pltpu.SemaphoreType.DMA((2, depth)),
        ],
        flops=10 * size,
    )


def solution(mesh):
    count = mesh.shape["px"]
    inner = 4 if count % 4 == 0 else 1
    split = Mesh(
        mesh.devices.reshape(mesh.shape["layer"], count // inner, inner, mesh.shape["py"]),
        ALL,
    )
    spec = P("layer", PX, "py")
    return jax.shard_map(
        lambda *a: tuple(shards(*a)),
        mesh=split,
        in_specs=(spec,) * 6,
        out_specs=(spec, spec),
        check_vma=False,
    )
```

```python
import functools

import jax
import jax.numpy as jnp
from jax import lax
from jax.experimental import pallas as pl
from jax.experimental.pallas import tpu as pltpu
from jax.sharding import Mesh
from jax.sharding import PartitionSpec as P


RIGHT, ROW, COL, VIA, GROUND = range(5)
FIELDS = 5
EARLY = (RIGHT, ROW, COL)
SUB, LANE = 8, 128
INNER, IMAGE, DOTS, FINAL = 3, 2, 2, 4
PX = ("px_0", "px_1")
ALL = ("layer", "px_0", "px_1", "py")


def lanes(shape):
    return lax.broadcasted_iota(jnp.int32, shape, len(shape) - 1)


def sublanes(shape):
    return lax.broadcasted_iota(jnp.int32, shape, len(shape) - 2)


def tile(index):
    if isinstance(index, int):
        return slice(index * SUB, (index + 1) * SUB)
    return pl.ds(pl.multiple_of(index * SUB, SUB), SUB)


def position():
    px = lax.axis_index("px_0") * lax.axis_size("px_1") + lax.axis_index("px_1")
    return (lax.axis_index("layer"), px, lax.axis_index("py"))


def sweep(low, high, several, body, carry=()):
    steps = (high - low) // several

    def step(i, carry):
        for j in range(several):
            carry = body(low + i * several + j, carry)
        return carry

    carry = lax.fori_loop(0, steps, step, carry)
    for t in range(low + steps * several, high):
        carry = body(t, carry)
    return carry


def spec_of(kind):
    return pl.BlockSpec(memory_space=kind)


def call(body, operands, kinds, outs, scratch=(), alias=None, flops=0, moved=0, limit=8 << 20):
    shapes = [
        pltpu.VMEM(o, jnp.float32) if isinstance(o, tuple) else o for o in outs
    ]
    operands = [
        pltpu.with_memory_space_constraint(o, k) for o, k in zip(operands, kinds)
    ]
    return pl.pallas_call(
        body,
        out_shape=shapes,
        in_specs=[spec_of(k) for k in kinds],
        out_specs=[spec_of(pltpu.VMEM if isinstance(o, tuple) else pltpu.HBM) for o in outs],
        scratch_shapes=list(scratch),
        input_output_aliases=alias or {},
        compiler_params=pltpu.CompilerParams(vmem_limit_bytes=limit),
        cost_estimate=pl.CostEstimate(flops=flops, bytes_accessed=moved, transcendentals=0),
    )(*operands)


def layer_of(core, k, depth):
    return jnp.where(core == 0, k, depth - 1 - k)


def link_of(core, k, depth):
    upper = depth - 1 if k == depth - 1 else depth - 2 - k
    return jnp.where(core == 0, k, upper)


def start_copies(core, depth, rows, sources, targets, masks, sem, slot, low, high, start, fields):
    copies = []
    for k in range(depth):
        at, link = layer_of(core, k, depth), link_of(core, k, depth)
        for f in fields:
            into = (
                masks.at[k, :, start : start + high - low]
                if f == FIELDS
                else targets[f].at[k, 0:rows, low:high]
            )
            source = sources[f].at[link if f in (VIA, FIELDS) else at, :, low:high]
            copy = pltpu.make_async_copy(source, into, sem.at[slot, f, k])
            copy.start()
            copies.append(copy)
    return copies


def masked(core, depth, layers, t, via, masks, low, high, start):
    for k in layers:
        value = via[k, tile(t), low:high] * masks[k, tile(t), start : start + high - low].astype(
            jnp.float32
        )
        if k == depth - 1:
            value = value * jnp.where(core == 0, 1.0, 0.0).astype(jnp.float32)
        via[k, tile(t), low:high] = value


def load_kernel(depth, rows, cols, *refs):
    sources, e = refs[0:6], refs[6:11]
    msg_right, msg_left, masks, pack, sem = refs[11:]
    core, _, _ = position()
    last = cols - LANE
    every = range(FIELDS + 1)
    begin = functools.partial(start_copies, core, depth, rows, sources, e, masks, sem)
    edges = begin(0, 0, LANE, 0, every) + begin(1, last, cols, LANE, every)
    others = begin(2, LANE, last, 0, EARLY)
    for copy in edges:
        copy.wait()
    lane = lanes((SUB, LANE))

    def body(t, carry):
        masked(core, depth, range(depth), t, e[VIA], masks, 0, LANE, 0)
        masked(core, depth, range(depth), t, e[VIA], masks, last, cols, LANE)
        to_right = jnp.zeros((SUB, LANE), jnp.float32)
        to_left = jnp.zeros((SUB, LANE), jnp.float32)
        for f in range(FIELDS):
            for k in range(depth):
                q = f * depth + k
                tail = e[f][k, tile(t), last:cols]
                head = e[f][k, tile(t), 0:LANE]
                if f == GROUND:
                    across = pltpu.roll(e[COL][k, tile(t), last:cols], 1, 1)
                    tail = tail + jnp.where(lane == LANE - 2, across, 0.0)
                shift = 4 * q + 2
                to_right = jnp.where((lane // 2) == 2 * q, pltpu.roll(tail, shift, 1), to_right)
                to_left = jnp.where((lane // 2) == 2 * q + 1, pltpu.roll(head, shift, 1), to_left)
        pack[0, tile(t), :] = to_right
        pack[1, tile(t), :] = to_left
        return carry

    sweep(0, rows // SUB, 4, body)
    used = msg_right.shape[0]
    msg_right[...] = pack[0].T[0:used]
    msg_left[...] = pack[1].T[0:used]
    for copy in others:
        copy.wait()


def middle_kernel(depth, rows, cols, *refs):
    sources, e, masks, sem = refs[0:6], refs[11:16], refs[16], refs[17]
    core, _, _ = position()
    low, high = LANE, cols - LANE
    begin = functools.partial(start_copies, core, depth, rows, sources, e, masks, sem, 0, low, high, 0)
    vias = begin((VIA, FIELDS))
    others = begin([f for f in range(FIELDS) if f not in EARLY and f != VIA])
    for k in range(depth):
        for copy in vias[2 * k : 2 * k + 2]:
            copy.wait()

        def body(t, carry, k=k):
            masked(core, depth, (k,), t, e[VIA], masks, low, high, 0)
            return carry

        sweep(0, rows // SUB, 4, body)
    for copy in others:
        copy.wait()


def unpack_columns(depth, cols, keep, t, both, e):
    value = both[tile(t), :]
    for f in range(FIELDS):
        for k in range(depth):
            got = pltpu.roll(value, (LANE - (4 * (f * depth + k) + 2)) % LANE, 1)
            fill = 1.0 if f == GROUND else 0.0
            e[f][k, tile(t), cols : cols + LANE] = jnp.where(keep, got, fill)


def kept_columns(places):
    _, _, py = position()
    lane = lanes((SUB, LANE))
    return ((lane < 2) & (py < places - 1)) | ((lane >= LANE - 2) & (py > 0))


def column_kernel(depth, rows, cols, places, *refs):
    from_left, from_right = refs[5:7]
    e = refs[7:12]
    msg_down, msg_up, both = refs[12:15]
    used = from_left.shape[0]
    both[...] = jnp.zeros_like(both)
    both[0:used] = from_left[...] + from_right[...]
    both[...] = both[...].T
    keep = kept_columns(places)
    unpack_columns(depth, cols, keep, 0, both, e)
    unpack_columns(depth, cols, keep, rows // SUB - 1, both, e)
    wide = cols + LANE
    sub = sublanes((SUB, wide))
    end = rows - SUB
    down = up = None
    for f in range(FIELDS):
        for k in range(depth):
            q = f * depth + k
            i = q % 4
            tail = e[f][k, end:rows, :]
            head = e[f][k, 0:SUB, :]
            if f == GROUND:
                across = pltpu.roll(e[ROW][k, end:rows, :], 1, 0)
                tail = tail + jnp.where(sub == SUB - 2, across, 0.0)
            tail = pltpu.roll(tail, (2 * i + 2) % SUB, 0)
            head = pltpu.roll(head, (2 * i) % SUB, 0)
            if i == 0:
                down, up = tail, head
            else:
                down = jnp.where(sub // 2 == i, tail, down)
                up = jnp.where(sub // 2 == i, head, up)
            if i == 3:
                msg_down[(q // 4) * SUB : (q // 4 + 1) * SUB, :] = down
                msg_up[(q // 4) * SUB : (q // 4 + 1) * SUB, :] = up


def eliminate(depth, rows, cols, places, t, e, fwd, gain, inv, out, slot):
    core, _, py = position()
    upper = core == 1
    count = rows // SUB + 1
    sub = sublanes((SUB, cols + LANE))
    before = jnp.where(t == 0, count - 1, t - 1)
    g = f = v = None
    for k in range(depth):
        row = e[ROW][k, tile(t), :]
        col = e[COL][k, tile(t), :]
        row_upper = pltpu.roll(jnp.where(sub == SUB - 1, e[ROW][k, tile(before), :], row), 1, 0)
        pivot = e[GROUND][k, tile(t), :] + row + row_upper + col + pltpu.roll(col, 1, 1)
        value = e[RIGHT][k, tile(t), :]
        if k:
            pivot = pivot + v * (1.0 - g)
            value = value + v * f
        v = e[VIA][k, tile(t), :]
        inverse = 1.0 / (pivot + v)
        g = v * inverse
        if k < depth - 1:
            f = value * inverse
            fwd[k, tile(t), :] = f
            gain[k, tile(t), :] = g
            inv[k, tile(t), :] = inverse
        else:
            inverse = jnp.where(upper, 0.0, inverse)
            fwd[k, tile(t), :] = value * inverse
            inv[k, tile(t), :] = inverse
            out[1, tile(slot), :] = jnp.where(upper, pivot, v * (1.0 - g))
            g = jnp.where(upper, 1.0, g)
            gain[k, tile(t), :] = g
            out[0, tile(slot), :] = g * value
    edge = (lanes((SUB, LANE)) == LANE - 1) & (py == places[1] - 1)
    for k in range(depth):
        part = e[COL][k, tile(t), cols - LANE : cols]
        e[COL][k, tile(t), cols - LANE : cols] = jnp.where(edge, 0.0, part)


def close_rows(depth, rows, places, e):
    _, px, _ = position()
    end = slice(rows - SUB, rows)
    for k in range(depth):
        row = e[ROW][k, end, :]
        edge = (sublanes(row.shape) == SUB - 1) & (px == places[0] - 1)
        e[ROW][k, end, :] = jnp.where(edge, 0.0, row)


def inner_kernel(depth, rows, cols, places, *refs):
    both, e, (fwd, gain, inv, out) = refs[5], refs[6:11], refs[11:15]
    keep = kept_columns(places[1])
    last = rows // SUB - 1

    def unpack(t, carry):
        unpack_columns(depth, cols, keep, t, both, e)
        return carry

    def body(t, carry):
        eliminate(depth, rows, cols, places, t, e, fwd, gain, inv, out, t - 1)
        return carry

    sweep(1, last, 2, unpack)
    sweep(1, last + 1, INNER, body)


def outer_kernel(depth, rows, cols, places, *refs):
    from_above, from_below = refs[8:10]
    e, (fwd, gain, inv, out) = refs[10:15], refs[15:19]
    _, px, _ = position()
    sub = sublanes((SUB, cols + LANE))
    top = (sub >= SUB - 2) & (px > 0)
    low = (sub < 2) & (px < places[0] - 1)
    for f in range(FIELDS):
        for k in range(depth):
            q = f * depth + k
            i = q % 4
            m = (q // 4) * SUB
            above = pltpu.roll(from_above[m : m + SUB, :], (SUB - 2 - 2 * i) % SUB, 0)
            under = pltpu.roll(from_below[m : m + SUB, :], (SUB - 2 * i) % SUB, 0)
            fill = 1.0 if f == GROUND else 0.0
            e[f][k, rows : rows + SUB, :] = jnp.where(top, above, jnp.where(low, under, fill))

    eliminate(depth, rows, cols, places, 0, e, fwd, gain, inv, out, 0)
    eliminate(depth, rows, cols, places, rows // SUB, e, fwd, gain, inv, out, 1)
    close_rows(depth, rows, places, e)


def back(depth, t, fwd, gain, middle, out):
    value = middle
    for k in range(depth - 1, -1, -1):
        value = fwd[k, tile(t), :] + gain[k, tile(t), :] * value
        out[k, tile(t), :] = value


def neighbours(k, t, count, sub, field, row, col):
    nxt = jnp.where(t == count - 1, 0, t + 1)
    pre = jnp.where(t == 0, count - 1, t - 1)
    r = row[k, tile(t), :]
    c = col[k, tile(t), :]
    z = field[k, tile(t), :]
    down = pltpu.roll(jnp.where(sub == 0, field[k, tile(nxt), :], z), SUB - 1, 0)
    flow = row[k, tile(pre), :] * field[k, tile(pre), :]
    up = pltpu.roll(jnp.where(sub == SUB - 1, flow, r * z), 1, 0)
    total = r * down + up + c * pltpu.roll(z, z.shape[1] - 1, 1) + pltpu.roll(c * z, 1, 1)
    return (total, z)


def join(depth, t, slot, fwd, gain, mine, theirs, inv4, z):
    ratio = 1.0 / (mine[1, tile(slot), :] + theirs[1, tile(slot), :])
    inv4[tile(t), :] = ratio
    back(depth, t, fwd, gain, (mine[0, tile(slot), :] + theirs[0, tile(slot), :]) * ratio, z)


def inner_solve_kernel(depth, rows, *refs):
    (fwd, gain, mine, theirs, z, inv4) = refs

    def body(t, carry):
        join(depth, t, t - 1, fwd, gain, mine, theirs, inv4, z)
        return carry

    sweep(1, rows // SUB, 3, body)


def image_kernel(depth, rows, cols, *refs):
    (right, row, col, via, fwd, gain, inv, mine, theirs, _, _, z, inv4, w, fwd2, out) = refs
    count = rows // SUB + 1
    sub = sublanes((SUB, cols + LANE))
    join(depth, 0, 0, fwd, gain, mine, theirs, inv4, z)
    join(depth, count - 1, 1, fwd, gain, mine, theirs, inv4, z)

    def body(t, carry):
        f = None
        for k in range(depth):
            total, _ = neighbours(k, t, count, sub, z, row, col)
            value = right[k, tile(t), :] - total
            w[k, tile(t), :] = value
            if k:
                value = value + via[k - 1, tile(t), :] * f
            f = value * inv[k, tile(t), :]
            fwd2[k, tile(t), :] = f
            if k == depth - 1:
                out[tile(t), :] = gain[k, tile(t), :] * value
        return carry

    sweep(0, count, IMAGE, body)


def gathered(sums, parts):
    lane = lanes(sums.shape)
    result = jnp.zeros(sums.shape, jnp.float32)
    for i, part in enumerate(parts):
        total = jnp.sum(jnp.sum(part, axis=0, keepdims=True), axis=1, keepdims=True)
        result = jnp.where(lane == i, total, result)
    return result


def early_kernel(depth, rows, cols, *refs):
    (right, z, w, acc) = refs

    def body(t, carry):
        rho, c = carry
        for k in range(depth):
            zz = z[k, tile(t), 0:cols]
            rho = rho + right[k, tile(t), 0:cols] * zz
            c = c + zz * w[k, tile(t), 0:cols]
        return (rho, c)

    zero = jnp.zeros((SUB, cols), jnp.float32)
    acc[0], acc[1] = sweep(0, rows // SUB, 2, body, (zero, zero))


def dots_kernel(depth, rows, cols, *refs):
    (row, col, fwd2, gain, mine, theirs, inv4, w, early, y, v, sums) = refs
    count = rows // SUB + 1
    wide = cols + LANE
    sub = sublanes((SUB, wide))

    def solve(t):
        back(depth, t, fwd2, gain, (mine[tile(t), :] + theirs[tile(t), :]) * inv4[tile(t), :], y)

    solve(count - 1)
    solve(0)

    def body(t, carry):
        e, g = carry
        solve(t + 1)
        for k in range(depth):
            total, yy = neighbours(k, t, count, sub, y, row, col)
            yy = yy[:, 0:cols]
            first = w[k, tile(t), 0:cols]
            second = first - total[:, 0:cols]
            v[k, tile(t), :] = second
            e = e + first * yy
            g = g + yy * second
        return (e, g)

    zero = jnp.zeros((SUB, cols), jnp.float32)
    e, g = sweep(0, count - 1, DOTS, body, (zero, zero))
    sums[...] = gathered(sums, (early[0], early[1], e, g))


def final_kernel(depth, rows, cols, *refs):
    (sums, right, z, w, y, v, x_out, r_out, x, r, sem) = refs
    core, _, _ = position()
    total = jnp.sum(sums[...], axis=0, keepdims=True)
    lane = lanes(total.shape)
    rho, c, e, g = (
        jnp.sum(jnp.where(lane == i, total, 0.0), axis=1, keepdims=True) for i in range(4)
    )
    alpha = rho / c
    rho1 = alpha * (alpha * e - c)
    beta = rho1 / rho
    curvature = c - 2.0 * alpha * e + alpha * alpha * g
    alpha1 = rho1 / (curvature - beta * rho1 / alpha)
    near = jnp.broadcast_to(alpha + alpha1 * (1.0 + beta), (SUB, cols))
    far = jnp.broadcast_to(alpha1 * alpha, (SUB, cols))
    copies = []
    for k in range(depth):

        def body(t, carry, k=k):
            x[k, tile(t), :] = near * z[k, tile(t), 0:cols] - far * y[k, tile(t), 0:cols]
            r[k, tile(t), :] = (
                right[k, tile(t), 0:cols] - near * w[k, tile(t), 0:cols] + far * v[k, tile(t), :]
            )
            return carry

        sweep(0, rows // SUB, FINAL, body)
        at = layer_of(core, k, depth)
        for slot, (value, target) in enumerate(((x, x_out), (r, r_out))):
            copy = pltpu.make_async_copy(value.at[k], target.at[at], sem.at[slot, k])
            copy.start()
            copies.append(copy)
    for copy in copies:
        copy.wait()


def shift(value, axis, by):
    count = lax.axis_size(axis)
    return lax.ppermute(value, axis, [(i, (i + by) % count) for i in range(count)])


def shards(right_side, row_conduct, column_conduct, via_conduct, via_mask, ground_conduct):
    depth, rows, cols = right_side.shape
    places = (lax.axis_size(PX), lax.axis_size("py"))
    devices = lax.axis_size(ALL)
    tall, wide = rows + SUB, cols + LANE
    ext = (depth, tall, wide)
    vmem, hbm = pltpu.VMEM, pltpu.HBM
    size = depth * tall * wide
    part = functools.partial

    inputs = [right_side, row_conduct, column_conduct, via_conduct, ground_conduct, via_mask]
    strips = (FIELDS * depth * 4, LANE)
    *e, msg_right, msg_left = call(
        part(load_kernel, depth, rows, cols),
        inputs,
        [hbm] * 6,
        [ext] * FIELDS + [strips] * 2,
        [
            pltpu.VMEM((depth, rows, 2 * LANE), jnp.int32),
            pltpu.VMEM((2, rows, LANE), jnp.float32),
            pltpu.SemaphoreType.DMA((3, 6, depth)),
        ],
        flops=size,
        moved=6 * size,
    )
    from_left = shift(msg_right, "py", 1)
    from_right = shift(msg_left, "py", -1)
    e = call(
        part(middle_kernel, depth, rows, cols),
        [*inputs, *e],
        [hbm] * 6 + [vmem] * FIELDS,
        [ext] * FIELDS,
        [
            pltpu.VMEM((depth, rows, cols - 2 * LANE), jnp.int32),
            pltpu.SemaphoreType.DMA((1, 6, depth)),
        ],
        alias={6 + i: i for i in range(FIELDS)},
        flops=10 * size,
        moved=18 * size,
    )
    strips = (FIELDS * depth * 2, wide)
    *e, msg_down, msg_up, both = call(
        part(column_kernel, depth, rows, cols, places[1]),
        [*e, from_left, from_right],
        [vmem] * 7,
        [ext] * FIELDS + [strips] * 2 + [(rows, LANE)],
        alias={i: i for i in range(FIELDS)},
        flops=size,
    )
    from_above = shift(msg_down, PX, 1)
    from_below = shift(msg_up, PX, -1)
    *state, mine = call(
        part(inner_kernel, depth, rows, cols, places),
        [*e, both],
        [vmem] * 6,
        [ext] * FIELDS + [ext] * 3 + [(2, rows - SUB, wide)],
        alias={i: i for i in range(FIELDS)},
        flops=30 * size,
    )
    theirs = shift(mine, "layer", 1)
    *e, fwd, gain, inv, mine_outer = call(
        part(outer_kernel, depth, rows, cols, places),
        [*state, from_above, from_below],
        [vmem] * 10,
        [ext] * FIELDS + [ext] * 3 + [(2, 2 * SUB, wide)],
        alias={i: i for i in range(FIELDS + 3)},
        flops=3 * size,
    )
    right, row, col, via, _ = e
    theirs_outer = shift(mine_outer, "layer", 1)
    z, inv4 = call(
        part(inner_solve_kernel, depth, rows),
        [fwd, gain, mine, theirs],
        [vmem] * 4,
        [ext, (tall, wide)],
        flops=8 * size,
    )
    z, inv4, w, fwd2, mine2 = call(
        part(image_kernel, depth, rows, cols),
        [right, row, col, via, fwd, gain, inv, mine_outer, theirs_outer, z, inv4],
        [vmem] * 11,
        [ext, (tall, wide)] + [ext] * 2 + [(tall, wide)],
        alias={9: 0, 10: 1},
        flops=30 * size,
    )
    theirs2 = shift(mine2, "layer", 1)
    (early,) = call(
        part(early_kernel, depth, rows, cols),
        [right, z, w],
        [vmem] * 3,
        [(2, SUB, cols)],
        flops=4 * size,
    )
    y, v, sums = call(
        part(dots_kernel, depth, rows, cols),
        [row, col, fwd2, gain, mine2, theirs2, inv4, w, early],
        [vmem] * 9,
        [ext, (depth, rows, cols), (devices, LANE)],
        flops=20 * size,
    )
    sums = lax.all_to_all(sums.reshape(devices, 1, LANE), ALL, 0, 0).reshape(devices, LANE)
    block = jax.ShapeDtypeStruct((depth, rows, cols), jnp.float32)
    return call(
        part(final_kernel, depth, rows, cols),
        [sums, right, z, w, y, v],
        [vmem] * 6,
        [block] * 2,
        [
            pltpu.VMEM((depth, rows, cols), jnp.float32),
            pltpu.VMEM((depth, rows, cols), jnp.float32),
            pltpu.SemaphoreType.DMA((2, depth)),
        ],
        flops=10 * size,
    )


def solution(mesh):
    count = mesh.shape["px"]
    inner = 4 if count % 4 == 0 else 1
    split = Mesh(
        mesh.devices.reshape(mesh.shape["layer"], count // inner, inner, mesh.shape["py"]),
        ALL,
    )
    spec = P("layer", PX, "py")

    def step(*arrays):
        return tuple(shards(*arrays))

    return jax.shard_map(
        step,
        mesh=split,
        in_specs=(spec,) * 6,
        out_specs=(spec, spec),
        check_vma=False,
    )
```

```python
import functools

import jax
import jax.numpy as jnp
from jax import lax
from jax.experimental import pallas as pl
from jax.experimental.pallas import tpu as pltpu
from jax.sharding import Mesh
from jax.sharding import PartitionSpec as P


RIGHT, ROW, COL, VIA, GROUND = range(5)
FIELDS = 5
EARLY = (RIGHT, ROW)
SUB, LANE = 8, 128
INNER, IMAGE, DOTS, FINAL = 3, 3, 3, 2
PX = ("px_0", "px_1")
ALL = ("layer", "px_0", "px_1", "py")


def lanes(shape):
    return lax.broadcasted_iota(jnp.int32, shape, len(shape) - 1)


def sublanes(shape):
    return lax.broadcasted_iota(jnp.int32, shape, len(shape) - 2)


def tile(index):
    if isinstance(index, int):
        return slice(index * SUB, (index + 1) * SUB)
    return pl.ds(pl.multiple_of(index * SUB, SUB), SUB)


def position():
    px = lax.axis_index("px_0") * lax.axis_size("px_1") + lax.axis_index("px_1")
    return (lax.axis_index("layer"), px, lax.axis_index("py"))


def sweep(low, high, several, body, carry=()):
    steps = (high - low) // several
    carry = lax.fori_loop(
        0, steps, lambda i, carry: body(low + i * several, several, carry), carry
    )
    left = high - low - steps * several
    return body(high - left, left, carry) if left else carry


def each(body):
    def run(t, n, carry):
        for i in range(n):
            carry = body(t + i, carry)
        return carry

    return run


def spec_of(kind):
    return pl.BlockSpec(memory_space=kind)


def call(body, operands, kinds, outs, scratch=(), alias=None, flops=0, moved=0, limit=8 << 20):
    shapes = [
        pltpu.VMEM(o, jnp.float32) if isinstance(o, tuple) else o for o in outs
    ]
    operands = [
        pltpu.with_memory_space_constraint(o, k) for o, k in zip(operands, kinds)
    ]
    return pl.pallas_call(
        body,
        out_shape=shapes,
        in_specs=[spec_of(k) for k in kinds],
        out_specs=[spec_of(pltpu.VMEM if isinstance(o, tuple) else pltpu.HBM) for o in outs],
        scratch_shapes=list(scratch),
        input_output_aliases=alias or {},
        compiler_params=pltpu.CompilerParams(vmem_limit_bytes=limit),
        cost_estimate=pl.CostEstimate(flops=flops, bytes_accessed=moved, transcendentals=0),
    )(*operands)


def layer_of(core, k, depth):
    return jnp.where(core == 0, k, depth - 1 - k)


def link_of(core, k, depth):
    upper = depth - 1 if k == depth - 1 else depth - 2 - k
    return jnp.where(core == 0, k, upper)


def start_copies(core, depth, rows, sources, targets, masks, sem, slot, low, high, start, fields):
    copies = []
    for k in range(depth):
        at, link = layer_of(core, k, depth), link_of(core, k, depth)
        for f in fields:
            into = (
                masks.at[k, :, start : start + high - low]
                if f == FIELDS
                else targets[f].at[k, 0:rows, low:high]
            )
            source = sources[f].at[link if f in (VIA, FIELDS) else at, :, low:high]
            copy = pltpu.make_async_copy(source, into, sem.at[slot, f, k])
            copy.start()
            copies.append(copy)
    return copies


def masked(core, depth, layers, t, via, masks, low, high, start):
    for k in layers:
        value = via[k, tile(t), low:high] * masks[k, tile(t), start : start + high - low].astype(
            jnp.float32
        )
        if k == depth - 1:
            value = value * jnp.where(core == 0, 1.0, 0.0).astype(jnp.float32)
        via[k, tile(t), low:high] = value


def load_kernel(depth, rows, cols, *refs):
    sources, e = refs[0:6], refs[6:11]
    msg_right, msg_left, masks, pack, sem = refs[11:]
    core, _, _ = position()
    last = cols - LANE
    every = range(FIELDS + 1)
    begin = functools.partial(start_copies, core, depth, rows, sources, e, masks, sem)
    edges = begin(0, 0, LANE, 0, every) + begin(1, last, cols, LANE, every)
    others = begin(2, LANE, last, 0, EARLY)
    for copy in edges:
        copy.wait()

    def mask(t, carry):
        masked(core, depth, range(depth), t, e[VIA], masks, 0, LANE, 0)
        masked(core, depth, range(depth), t, e[VIA], masks, last, cols, LANE)
        return carry

    sweep(0, rows // SUB, 4, each(mask))
    several = 2 * SUB
    lane = lanes((several, LANE))
    pair = lane // 2

    def place(i, _):
        at = pl.ds(pl.multiple_of(i * several, several), several)
        to_right = jnp.zeros((several, LANE), jnp.float32)
        to_left = jnp.zeros((several, LANE), jnp.float32)
        for f in range(FIELDS):
            for k in range(depth):
                q = f * depth + k
                tail = e[f][k, at, last:cols]
                head = e[f][k, at, 0:LANE]
                if f == GROUND:
                    across = pltpu.roll(e[COL][k, at, last:cols], 1, 1)
                    tail = tail + jnp.where(lane == LANE - 2, across, 0.0)
                shift = 4 * q + 2
                to_right = jnp.where(pair == 2 * q, pltpu.roll(tail, shift, 1), to_right)
                to_left = jnp.where(pair == 2 * q + 1, pltpu.roll(head, shift, 1), to_left)
        pack[0, at, :] = to_right
        pack[1, at, :] = to_left
        return 0

    lax.fori_loop(0, rows // several, place, 0)
    used = msg_right.shape[0]
    msg_right[...] = pack[0].T[0:used]
    msg_left[...] = pack[1].T[0:used]
    for copy in others:
        copy.wait()


def middle_kernel(depth, rows, cols, *refs):
    sources, e, masks, sem = refs[0:6], refs[11:16], refs[16], refs[17]
    core, _, _ = position()
    low, high = LANE, cols - LANE
    begin = functools.partial(start_copies, core, depth, rows, sources, e, masks, sem, 0, low, high, 0)
    vias = begin((VIA, FIELDS))
    others = begin([f for f in range(FIELDS) if f not in EARLY and f != VIA])
    for k in range(depth):
        for copy in vias[2 * k : 2 * k + 2]:
            copy.wait()

        def body(t, carry, k=k):
            masked(core, depth, (k,), t, e[VIA], masks, low, high, 0)
            return carry

        sweep(0, rows // SUB, 4, each(body))
    for copy in others:
        copy.wait()


def unpack_columns(depth, cols, keep, t, both, e):
    value = both[tile(t), :]
    for f in range(FIELDS):
        for k in range(depth):
            got = pltpu.roll(value, (LANE - (4 * (f * depth + k) + 2)) % LANE, 1)
            fill = 1.0 if f == GROUND else 0.0
            e[f][k, tile(t), cols : cols + LANE] = jnp.where(keep, got, fill)


def kept_columns(places):
    _, _, py = position()
    lane = lanes((SUB, LANE))
    return ((lane < 2) & (py < places - 1)) | ((lane >= LANE - 2) & (py > 0))


def column_kernel(depth, rows, cols, places, *refs):
    from_left, from_right = refs[5:7]
    e = refs[7:12]
    msg_down, msg_up, both = refs[12:15]
    used = from_left.shape[0]
    both[...] = jnp.zeros_like(both)
    both[0:used] = from_left[...] + from_right[...]
    both[...] = both[...].T
    keep = kept_columns(places)
    unpack_columns(depth, cols, keep, 0, both, e)
    unpack_columns(depth, cols, keep, rows // SUB - 1, both, e)
    wide = cols + LANE
    sub = sublanes((SUB, wide))
    end = rows - SUB
    down = up = None
    for f in range(FIELDS):
        for k in range(depth):
            q = f * depth + k
            i = q % 4
            tail = e[f][k, end:rows, :]
            head = e[f][k, 0:SUB, :]
            if f == GROUND:
                across = pltpu.roll(e[ROW][k, end:rows, :], 1, 0)
                tail = tail + jnp.where(sub == SUB - 2, across, 0.0)
            tail = pltpu.roll(tail, (2 * i + 2) % SUB, 0)
            head = pltpu.roll(head, (2 * i) % SUB, 0)
            if i == 0:
                down, up = tail, head
            else:
                down = jnp.where(sub // 2 == i, tail, down)
                up = jnp.where(sub // 2 == i, head, up)
            if i == 3:
                msg_down[(q // 4) * SUB : (q // 4 + 1) * SUB, :] = down
                msg_up[(q // 4) * SUB : (q // 4 + 1) * SUB, :] = up


def eliminate(depth, rows, cols, places, t, e, fwd, gain, inv, out, slot):
    core, _, py = position()
    upper = core == 1
    count = rows // SUB + 1
    sub = sublanes((SUB, cols + LANE))
    before = jnp.where(t == 0, count - 1, t - 1)
    g = f = v = None
    for k in range(depth):
        row = e[ROW][k, tile(t), :]
        col = e[COL][k, tile(t), :]
        row_upper = pltpu.roll(jnp.where(sub == SUB - 1, e[ROW][k, tile(before), :], row), 1, 0)
        pivot = e[GROUND][k, tile(t), :] + row + row_upper + col + pltpu.roll(col, 1, 1)
        value = e[RIGHT][k, tile(t), :]
        if k:
            pivot = pivot + v * (1.0 - g)
            value = value + v * f
        v = e[VIA][k, tile(t), :]
        inverse = 1.0 / (pivot + v)
        g = v * inverse
        if k < depth - 1:
            f = value * inverse
            fwd[k, tile(t), :] = f
            gain[k, tile(t), :] = g
            inv[k, tile(t), :] = inverse
        else:
            inverse = jnp.where(upper, 0.0, inverse)
            fwd[k, tile(t), :] = value * inverse
            inv[k, tile(t), :] = inverse
            out[1, tile(slot), :] = jnp.where(upper, pivot, v * (1.0 - g))
            g = jnp.where(upper, 1.0, g)
            gain[k, tile(t), :] = g
            out[0, tile(slot), :] = g * value
    edge = (lanes((SUB, LANE)) == LANE - 1) & (py == places[1] - 1)
    for k in range(depth):
        part = e[COL][k, tile(t), cols - LANE : cols]
        e[COL][k, tile(t), cols - LANE : cols] = jnp.where(edge, 0.0, part)


def close_rows(depth, rows, places, e):
    _, px, _ = position()
    end = slice(rows - SUB, rows)
    for k in range(depth):
        row = e[ROW][k, end, :]
        edge = (sublanes(row.shape) == SUB - 1) & (px == places[0] - 1)
        e[ROW][k, end, :] = jnp.where(edge, 0.0, row)


def inner_kernel(depth, rows, cols, places, low, high, held, *refs):
    both, e, (fwd, gain, inv, out) = refs[FIELDS + held], refs[-9:-4], refs[-4:]
    keep = kept_columns(places[1])

    def unpack(t, carry):
        unpack_columns(depth, cols, keep, t, both, e)
        return carry

    def body(t, carry):
        eliminate(depth, rows, cols, places, t, e, fwd, gain, inv, out, t - low)
        return carry

    sweep(low, min(high, rows // SUB - 1), 2, each(unpack))
    sweep(low, high, INNER, each(body))


def outer_kernel(depth, rows, cols, places, *refs):
    from_above, from_below = refs[8:10]
    e, (fwd, gain, inv, out) = refs[10:15], refs[15:19]
    _, px, _ = position()
    sub = sublanes((SUB, cols + LANE))
    top = (sub >= SUB - 2) & (px > 0)
    low = (sub < 2) & (px < places[0] - 1)
    for f in range(FIELDS):
        for k in range(depth):
            q = f * depth + k
            i = q % 4
            m = (q // 4) * SUB
            above = pltpu.roll(from_above[m : m + SUB, :], (SUB - 2 - 2 * i) % SUB, 0)
            under = pltpu.roll(from_below[m : m + SUB, :], (SUB - 2 * i) % SUB, 0)
            fill = 1.0 if f == GROUND else 0.0
            e[f][k, rows : rows + SUB, :] = jnp.where(top, above, jnp.where(low, under, fill))

    eliminate(depth, rows, cols, places, 0, e, fwd, gain, inv, out, 0)
    eliminate(depth, rows, cols, places, rows // SUB, e, fwd, gain, inv, out, 1)
    close_rows(depth, rows, places, e)


def back(depth, t, fwd, gain, middle, out):
    value = middle
    for k in range(depth - 1, -1, -1):
        value = fwd[k, tile(t), :] + gain[k, tile(t), :] * value
        out[k, tile(t), :] = value


def stencil(k, t, n, count, sub, field, row, col):
    wrap = lambda i: i % count if isinstance(i, int) else i
    z = [field[k, tile(wrap(t + i)), :] for i in range(-1, n + 1)]
    r = [row[k, tile(wrap(t + i)), :] for i in range(-1, n)]
    flows = [a * b for a, b in zip(r, z)]
    totals = []
    for i in range(1, n + 1):
        here = z[i]
        c = col[k, tile(wrap(t + i - 1)), :]
        down = pltpu.roll(jnp.where(sub == 0, z[i + 1], here), SUB - 1, 0)
        up = pltpu.roll(jnp.where(sub == SUB - 1, flows[i - 1], flows[i]), 1, 0)
        across = pltpu.roll(here, here.shape[1] - 1, 1)
        totals.append(r[i] * down + up + c * across + pltpu.roll(c * here, 1, 1))
    return totals, z[1 : n + 1]


def join(depth, t, slot, fwd, gain, mine, theirs, inv4, z):
    ratio = 1.0 / (mine[1, tile(slot), :] + theirs[1, tile(slot), :])
    inv4[tile(t), :] = ratio
    back(depth, t, fwd, gain, (mine[0, tile(slot), :] + theirs[0, tile(slot), :]) * ratio, z)


def image_of(depth, t, n, count, sub, slots, refs):
    right, row, col, via, gain, inv, z, w, fwd2, out = refs
    wrap = lambda i: i % count if isinstance(i, int) else i
    f = [None] * n
    for k in range(depth):
        totals, _ = stencil(k, t, n, count, sub, z, row, col)
        for i in range(n):
            at = tile(wrap(t + i))
            value = right[k, at, :] - totals[i]
            w[k, at, :] = value
            if k:
                value = value + via[k - 1, at, :] * f[i]
            f[i] = value * inv[k, at, :]
            fwd2[k, at, :] = f[i]
            if k == depth - 1:
                out[tile(slots + i), :] = gain[k, at, :] * value


def inner_image_kernel(depth, rows, cols, low, high, first, *refs):
    right, row, col, via, fwd, gain, inv, mine, theirs = refs[0:9]
    z, inv4, w, fwd2, out = refs[-5:]
    count = rows // SUB + 1
    sub = sublanes((SUB, cols + LANE))

    def solve(t):
        join(depth, t, t - low, fwd, gain, mine, theirs, inv4, z)

    begin = low + 1 if first else low - 1
    for t in range(low, begin + 1):
        solve(t)

    def body(t, n, carry):
        for i in range(n):
            solve(t + 1 + i)
        image_of(
            depth, t, n, count, sub, t - 2, (right, row, col, via, gain, inv, z, w, fwd2, out)
        )
        return carry

    sweep(begin, high - 1, IMAGE, body)


def outer_image_kernel(depth, rows, cols, *refs):
    (right, row, col, via, fwd, gain, inv, mine, theirs) = refs[0:9]
    z, inv4, w, fwd2, out = refs[13:18]
    count = rows // SUB + 1
    sub = sublanes((SUB, cols + LANE))
    join(depth, 0, 0, fwd, gain, mine, theirs, inv4, z)
    join(depth, count - 1, 1, fwd, gain, mine, theirs, inv4, z)
    image_of(
        depth, count - 2, 4, count, sub, 0, (right, row, col, via, gain, inv, z, w, fwd2, out)
    )


def gathered(sums, parts):
    lane = lanes(sums.shape)
    result = jnp.zeros(sums.shape, jnp.float32)
    for i, part in enumerate(parts):
        total = jnp.sum(jnp.sum(part, axis=0, keepdims=True), axis=1, keepdims=True)
        result = jnp.where(lane == i, total, result)
    return result


def early_kernel(depth, rows, cols, *refs):
    (right, z, w, acc) = refs

    def body(t, carry):
        rho, c = carry
        for k in range(depth):
            zz = z[k, tile(t), 0:cols]
            rho = rho + right[k, tile(t), 0:cols] * zz
            c = c + zz * w[k, tile(t), 0:cols]
        return (rho, c)

    zero = jnp.zeros((SUB, cols), jnp.float32)
    acc[0], acc[1] = sweep(0, rows // SUB, 2, each(body), (zero, zero))


def second_image_of(depth, cols, t, n, count, sub, refs, carry):
    row, col, w, y, v = refs
    e, g = carry
    for k in range(depth):
        totals, fields = stencil(k, t, n, count, sub, y, row, col)
        for i in range(n):
            yy = fields[i][:, 0:cols]
            first = w[k, tile(t + i), 0:cols]
            second = first - totals[i][:, 0:cols]
            v[k, tile(t + i), :] = second
            e = e + first * yy
            g = g + yy * second
    return e, g


def inner_dots_kernel(depth, rows, cols, *refs):
    (row, col, fwd2, gain, mine, theirs, inv4, w, y, v, acc) = refs
    count = rows // SUB + 1
    sub = sublanes((SUB, cols + LANE))

    def solve(t):
        middle = (mine[tile(t - 2), :] + theirs[tile(t - 2), :]) * inv4[tile(t), :]
        back(depth, t, fwd2, gain, middle, y)

    solve(2)
    solve(3)

    def body(t, n, carry):
        for i in range(n):
            solve(t + 1 + i)
        return second_image_of(depth, cols, t, n, count, sub, (row, col, w, y, v), carry)

    zero = jnp.zeros((SUB, cols), jnp.float32)
    acc[0], acc[1] = sweep(3, count - 3, DOTS, body, (zero, zero))


def outer_dots_kernel(depth, rows, cols, *refs):
    (row, col, fwd2, gain, mine, theirs, inv4, w, early, acc) = refs[0:10]
    y, v, sums = refs[12:15]
    count = rows // SUB + 1
    sub = sublanes((SUB, cols + LANE))
    for slot, t in enumerate((count - 2, count - 1, 0, 1)):
        middle = (mine[tile(slot), :] + theirs[tile(slot), :]) * inv4[tile(t), :]
        back(depth, t, fwd2, gain, middle, y)
    carry = (acc[0], acc[1])
    for t, n in ((count - 3, 2), (0, 3)):
        carry = second_image_of(depth, cols, t, n, count, sub, (row, col, w, y, v), carry)
    sums[...] = gathered(sums, (early[0], early[1], *carry))


def final_kernel(depth, rows, cols, *refs):
    (sums, right, z, w, y, v, x_out, r_out, x, r, sem) = refs
    core, _, _ = position()
    total = jnp.sum(sums[...], axis=0, keepdims=True)
    lane = lanes(total.shape)
    rho, c, e, g = (
        jnp.sum(jnp.where(lane == i, total, 0.0), axis=1, keepdims=True) for i in range(4)
    )
    alpha = rho / c
    rho1 = alpha * (alpha * e - c)
    beta = rho1 / rho
    curvature = c - 2.0 * alpha * e + alpha * alpha * g
    alpha1 = rho1 / (curvature - beta * rho1 / alpha)
    near = jnp.broadcast_to(alpha + alpha1 * (1.0 + beta), (SUB, cols))
    far = jnp.broadcast_to(alpha1 * alpha, (SUB, cols))
    copies = []
    for k in range(depth):

        def body(t, carry, k=k):
            x[k, tile(t), :] = near * z[k, tile(t), 0:cols] - far * y[k, tile(t), 0:cols]
            r[k, tile(t), :] = (
                right[k, tile(t), 0:cols] - near * w[k, tile(t), 0:cols] + far * v[k, tile(t), :]
            )
            return carry

        sweep(0, rows // SUB, FINAL, each(body))
        at = layer_of(core, k, depth)
        for slot, (value, target) in enumerate(((x, x_out), (r, r_out))):
            copy = pltpu.make_async_copy(value.at[k], target.at[at], sem.at[slot, k])
            copy.start()
            copies.append(copy)
    for copy in copies:
        copy.wait()


def shift(value, axis, by):
    count = lax.axis_size(axis)
    return lax.ppermute(value, axis, [(i, (i + by) % count) for i in range(count)])


def shards(right_side, row_conduct, column_conduct, via_conduct, via_mask, ground_conduct):
    depth, rows, cols = right_side.shape
    places = (lax.axis_size(PX), lax.axis_size("py"))
    devices = lax.axis_size(ALL)
    tall, wide = rows + SUB, cols + LANE
    ext = (depth, tall, wide)
    vmem, hbm = pltpu.VMEM, pltpu.HBM
    size = depth * tall * wide
    part = functools.partial

    inputs = [right_side, row_conduct, column_conduct, via_conduct, ground_conduct, via_mask]
    strips = (FIELDS * depth * 4, LANE)
    *e, msg_right, msg_left = call(
        part(load_kernel, depth, rows, cols),
        inputs,
        [hbm] * 6,
        [ext] * FIELDS + [strips] * 2,
        [
            pltpu.VMEM((depth, rows, 2 * LANE), jnp.int32),
            pltpu.VMEM((2, rows, LANE), jnp.float32),
            pltpu.SemaphoreType.DMA((3, 6, depth)),
        ],
        flops=size,
        moved=6 * size,
    )
    from_left = shift(msg_right, "py", 1)
    from_right = shift(msg_left, "py", -1)
    e = call(
        part(middle_kernel, depth, rows, cols),
        [*inputs, *e],
        [hbm] * 6 + [vmem] * FIELDS,
        [ext] * FIELDS,
        [
            pltpu.VMEM((depth, rows, cols - 2 * LANE), jnp.int32),
            pltpu.SemaphoreType.DMA((1, 6, depth)),
        ],
        alias={6 + i: i for i in range(FIELDS)},
        flops=10 * size,
        moved=18 * size,
    )
    strips = (FIELDS * depth * 2, wide)
    *e, msg_down, msg_up, both = call(
        part(column_kernel, depth, rows, cols, places[1]),
        [*e, from_left, from_right],
        [vmem] * 7,
        [ext] * FIELDS + [strips] * 2 + [(rows, LANE)],
        alias={i: i for i in range(FIELDS)},
        flops=size,
    )
    from_above = shift(msg_down, PX, 1)
    from_below = shift(msg_up, PX, -1)
    end = rows // SUB
    split = end // 2 + 1
    flops = 15 * size
    *state, mine = call(
        part(inner_kernel, depth, rows, cols, places, 1, split, 0),
        [*e, both],
        [vmem] * 6,
        [ext] * FIELDS + [ext] * 3 + [(2, (split - 1) * SUB, wide)],
        alias={i: i for i in range(FIELDS)},
        flops=flops,
    )
    theirs = shift(mine, "layer", 1)
    *state, mine_rest = call(
        part(inner_kernel, depth, rows, cols, places, split, end, 3),
        [*state, both],
        [vmem] * 9,
        [ext] * FIELDS + [ext] * 3 + [(2, (end - split) * SUB, wide)],
        alias={i: i for i in range(FIELDS + 3)},
        flops=flops,
    )
    theirs_rest = shift(mine_rest, "layer", 1)
    right, row, col, via, _, fwd, gain, inv = state
    images = [ext, (tall, wide), ext, ext, (tall - 4 * SUB, wide)]
    images = call(
        part(inner_image_kernel, depth, rows, cols, 1, split, True),
        [right, row, col, via, fwd, gain, inv, mine, theirs],
        [vmem] * 9,
        images,
        flops=flops,
    )
    z, inv4, w, fwd2, mine2 = call(
        part(inner_image_kernel, depth, rows, cols, split, end, False),
        [right, row, col, via, fwd, gain, inv, mine_rest, theirs_rest, *images],
        [vmem] * 14,
        [ext, (tall, wide), ext, ext, (tall - 4 * SUB, wide)],
        alias={9 + i: i for i in range(5)},
        flops=flops,
    )
    *e, fwd, gain, inv, mine_outer = call(
        part(outer_kernel, depth, rows, cols, places),
        [*state, from_above, from_below],
        [vmem] * 10,
        [ext] * FIELDS + [ext] * 3 + [(2, 2 * SUB, wide)],
        alias={i: i for i in range(FIELDS + 3)},
        flops=3 * size,
    )
    right, row, col, via, _ = e
    theirs_outer = shift(mine_outer, "layer", 1)
    theirs2 = shift(mine2, "layer", 1)
    z, inv4, w, fwd2, mine2_outer = call(
        part(outer_image_kernel, depth, rows, cols),
        [right, row, col, via, fwd, gain, inv, mine_outer, theirs_outer, z, inv4, w, fwd2],
        [vmem] * 13,
        [ext, (tall, wide), ext, ext, (4 * SUB, wide)],
        alias={9: 0, 10: 1, 11: 2, 12: 3},
        flops=8 * size,
    )
    theirs2_outer = shift(mine2_outer, "layer", 1)
    (early,) = call(
        part(early_kernel, depth, rows, cols),
        [right, z, w],
        [vmem] * 3,
        [(2, SUB, cols)],
        flops=4 * size,
    )
    block = (depth, rows, cols)
    y, v, acc = call(
        part(inner_dots_kernel, depth, rows, cols),
        [row, col, fwd2, gain, mine2, theirs2, inv4, w],
        [vmem] * 8,
        [ext, block, (2, SUB, cols)],
        flops=20 * size,
    )
    y, v, sums = call(
        part(outer_dots_kernel, depth, rows, cols),
        [row, col, fwd2, gain, mine2_outer, theirs2_outer, inv4, w, early, acc, y, v],
        [vmem] * 12,
        [ext, block, (devices, LANE)],
        alias={10: 0, 11: 1},
        flops=8 * size,
    )
    sums = lax.all_to_all(sums.reshape(devices, 1, LANE), ALL, 0, 0).reshape(devices, LANE)
    result = jax.ShapeDtypeStruct(block, jnp.float32)
    return call(
        part(final_kernel, depth, rows, cols),
        [sums, right, z, w, y, v],
        [vmem] * 6,
        [result] * 2,
        [
            pltpu.VMEM((depth, rows, cols), jnp.float32),
            pltpu.VMEM((depth, rows, cols), jnp.float32),
            pltpu.SemaphoreType.DMA((2, depth)),
        ],
        flops=10 * size,
    )


def solution(mesh):
    count = mesh.shape["px"]
    inner = 4 if count % 4 == 0 else 1
    split = Mesh(
        mesh.devices.reshape(mesh.shape["layer"], count // inner, inner, mesh.shape["py"]),
        ALL,
    )
    spec = P("layer", PX, "py")

    def step(*arrays):
        return tuple(shards(*arrays))

    return jax.shard_map(
        step,
        mesh=split,
        in_specs=(spec,) * 6,
        out_specs=(spec, spec),
        check_vma=False,
    )
```

```python
import functools

import jax
import jax.numpy as jnp
from jax import lax
from jax.experimental import pallas as pl
from jax.experimental.pallas import tpu as pltpu
from jax.sharding import Mesh
from jax.sharding import PartitionSpec as P


RIGHT, ROW, COL, VIA, GROUND = range(5)
FIELDS = 5
EARLY = (RIGHT, ROW)
SUB, LANE = 8, 128
INNER, IMAGE, DOTS, FINAL = 4, 3, 4, 2
PX = ("px_0", "px_1")
ALL = ("layer", "px_0", "px_1", "py")


def lanes(shape):
    return lax.broadcasted_iota(jnp.int32, shape, len(shape) - 1)


def sublanes(shape):
    return lax.broadcasted_iota(jnp.int32, shape, len(shape) - 2)


def tile(index):
    if isinstance(index, int):
        return slice(index * SUB, (index + 1) * SUB)
    return pl.ds(pl.multiple_of(index * SUB, SUB), SUB)


def position():
    px = lax.axis_index("px_0") * lax.axis_size("px_1") + lax.axis_index("px_1")
    return (lax.axis_index("layer"), px, lax.axis_index("py"))


def sweep(low, high, several, body, carry=()):
    steps = (high - low) // several
    carry = lax.fori_loop(
        0, steps, lambda i, carry: body(low + i * several, several, carry), carry
    )
    left = high - low - steps * several
    return body(high - left, left, carry) if left else carry


def each(body):
    def run(t, n, carry):
        for i in range(n):
            carry = body(t + i, carry)
        return carry

    return run


def spec_of(kind):
    return pl.BlockSpec(memory_space=kind)


def call(body, operands, kinds, outs, scratch=(), alias=None, flops=0, moved=0, limit=8 << 20):
    shapes = [
        pltpu.VMEM(o, jnp.float32) if isinstance(o, tuple) else o for o in outs
    ]
    operands = [
        pltpu.with_memory_space_constraint(o, k) for o, k in zip(operands, kinds)
    ]
    return pl.pallas_call(
        body,
        out_shape=shapes,
        in_specs=[spec_of(k) for k in kinds],
        out_specs=[spec_of(pltpu.VMEM if isinstance(o, tuple) else pltpu.HBM) for o in outs],
        scratch_shapes=list(scratch),
        input_output_aliases=alias or {},
        compiler_params=pltpu.CompilerParams(vmem_limit_bytes=limit),
        cost_estimate=pl.CostEstimate(flops=flops, bytes_accessed=moved, transcendentals=0),
    )(*operands)


def layer_of(core, k, depth):
    return jnp.where(core == 0, k, depth - 1 - k)


def link_of(core, k, depth):
    upper = depth - 1 if k == depth - 1 else depth - 2 - k
    return jnp.where(core == 0, k, upper)


def start_copies(core, depth, rows, sources, targets, masks, sem, slot, low, high, start, fields):
    copies = []
    for k in range(depth):
        at, link = layer_of(core, k, depth), link_of(core, k, depth)
        for f in fields:
            into = (
                masks.at[k, :, start : start + high - low]
                if f == FIELDS
                else targets[f].at[k, 0:rows, low:high]
            )
            source = sources[f].at[link if f in (VIA, FIELDS) else at, :, low:high]
            copy = pltpu.make_async_copy(source, into, sem.at[slot, f, k])
            copy.start()
            copies.append(copy)
    return copies


def masked(core, depth, layers, t, via, masks, low, high, start):
    for k in layers:
        value = via[k, tile(t), low:high] * masks[k, tile(t), start : start + high - low].astype(
            jnp.float32
        )
        if k == depth - 1:
            value = value * jnp.where(core == 0, 1.0, 0.0).astype(jnp.float32)
        via[k, tile(t), low:high] = value


def load_kernel(depth, rows, cols, *refs):
    sources, e = refs[0:6], refs[6:11]
    msg_right, msg_left, masks, pack, sem = refs[11:]
    core, _, _ = position()
    last = cols - LANE
    begin = functools.partial(start_copies, core, depth, rows, sources, e, masks, sem)
    every = range(FIELDS + 1)
    edges = begin(0, 0, LANE, 0, every) + begin(1, last, cols, LANE, every)
    others = begin(2, LANE, last, 0, EARLY)
    for copy in edges:
        copy.wait()

    def mask(t, carry):
        masked(core, depth, range(depth), t, e[VIA], masks, 0, LANE, 0)
        masked(core, depth, range(depth), t, e[VIA], masks, last, cols, LANE)
        return carry

    sweep(0, rows // SUB, 4, each(mask))
    several = 8 * SUB
    lane = lanes((several, LANE))
    pair = lane // 2

    def place(i, _):
        at = pl.ds(pl.multiple_of(i * several, several), several)
        to_right = to_left = jnp.zeros((several, LANE), jnp.float32)
        for f in range(FIELDS):
            for k in range(depth):
                q = f * depth + k
                tail = e[f][k, at, last:cols]
                head = e[f][k, at, 0:LANE]
                if f == GROUND:
                    across = pltpu.roll(e[COL][k, at, last:cols], 1, 1)
                    tail = tail + jnp.where(lane == LANE - 2, across, 0.0)
                if q:
                    head = pltpu.roll(head, 2 * q, 1)
                to_right = jnp.where(pair == q, pltpu.roll(tail, 2 * q + 2, 1), to_right)
                to_left = jnp.where(pair == q, head, to_left)
        pack[0, at, :] = to_right
        pack[1, at, :] = to_left
        return 0

    lax.fori_loop(0, rows // several, place, 0)
    used = msg_right.shape[0]
    msg_right[...] = pack[0].T[0:used]
    msg_left[...] = pack[1].T[0:used]
    for copy in others:
        copy.wait()


def middle_kernel(depth, rows, cols, *refs):
    sources, e, masks, sem = refs[0:6], refs[11:16], refs[16], refs[17]
    core, _, _ = position()
    low, high = LANE, cols - LANE
    begin = functools.partial(start_copies, core, depth, rows, sources, e, masks, sem, 0, low, high, 0)
    vias = begin((VIA, FIELDS))
    others = begin([f for f in range(FIELDS) if f not in EARLY and f != VIA])
    for k in range(depth):
        for copy in vias[2 * k : 2 * k + 2]:
            copy.wait()

        def body(t, carry, k=k):
            masked(core, depth, (k,), t, e[VIA], masks, low, high, 0)
            return carry

        sweep(0, rows // SUB, 4, each(body))
    for copy in others:
        copy.wait()


def unpack_columns(depth, cols, keep, t, both, e):
    value = both[tile(t), :]
    for f in range(FIELDS):
        for k in range(depth):
            got = pltpu.roll(value, (LANE - (4 * (f * depth + k) + 2)) % LANE, 1)
            fill = 1.0 if f == GROUND else 0.0
            e[f][k, tile(t), cols : cols + LANE] = jnp.where(keep, got, fill)


def kept_columns(places):
    _, _, py = position()
    lane = lanes((SUB, LANE))
    return ((lane < 2) & (py < places - 1)) | ((lane >= LANE - 2) & (py > 0))


def column_kernel(depth, rows, cols, places, *refs):
    from_left, from_right = refs[5:7]
    e = refs[7:12]
    msg_down, msg_up, both = refs[12:15]
    both[...] = jnp.zeros_like(both)
    part = sublanes((SUB, LANE)) // 2
    for m in range(from_left.shape[0] // SUB):
        left = from_left[m * SUB : (m + 1) * SUB, :]
        right = from_right[m * SUB : (m + 1) * SUB, :]
        turn = lambda x, by: pltpu.roll(x, by % SUB, 0) if by % SUB else x
        for half in range(2):
            back_by = -4 * half
            value = jnp.where(part == 0, turn(left, back_by), turn(right, 2 + back_by))
            value = jnp.where(part == 2, turn(left, 2 + back_by), value)
            value = jnp.where(part == 3, turn(right, 4 + back_by), value)
            at = (2 * m + half) * SUB
            both[at : at + SUB, :] = value
    both[...] = both[...].T
    keep = kept_columns(places)
    unpack_columns(depth, cols, keep, 0, both, e)
    unpack_columns(depth, cols, keep, rows // SUB - 1, both, e)
    wide = cols + LANE
    sub = sublanes((SUB, wide))
    end = rows - SUB
    down = up = None
    for f in range(FIELDS):
        for k in range(depth):
            q = f * depth + k
            i = q % 4
            tail = e[f][k, end:rows, :]
            head = e[f][k, 0:SUB, :]
            if f == GROUND:
                across = pltpu.roll(e[ROW][k, end:rows, :], 1, 0)
                tail = tail + jnp.where(sub == SUB - 2, across, 0.0)
            tail = pltpu.roll(tail, (2 * i + 2) % SUB, 0)
            head = pltpu.roll(head, (2 * i) % SUB, 0)
            if i == 0:
                down, up = tail, head
            else:
                down = jnp.where(sub // 2 == i, tail, down)
                up = jnp.where(sub // 2 == i, head, up)
            if i == 3:
                msg_down[(q // 4) * SUB : (q // 4 + 1) * SUB, :] = down
                msg_up[(q // 4) * SUB : (q // 4 + 1) * SUB, :] = up


def eliminate(depth, rows, cols, places, t, e, fwd, gain, inv, out, slot):
    core, _, py = position()
    upper = core == 1
    count = rows // SUB + 1
    sub = sublanes((SUB, cols + LANE))
    before = jnp.where(t == 0, count - 1, t - 1)
    g = f = v = None
    for k in range(depth):
        row = e[ROW][k, tile(t), :]
        col = e[COL][k, tile(t), :]
        row_upper = pltpu.roll(jnp.where(sub == SUB - 1, e[ROW][k, tile(before), :], row), 1, 0)
        pivot = e[GROUND][k, tile(t), :] + row + row_upper + col + pltpu.roll(col, 1, 1)
        value = e[RIGHT][k, tile(t), :]
        if k:
            pivot = pivot + v * (1.0 - g)
            value = value + v * f
        v = e[VIA][k, tile(t), :]
        inverse = 1.0 / (pivot + v)
        g = v * inverse
        if k < depth - 1:
            f = value * inverse
            fwd[k, tile(t), :] = f
            gain[k, tile(t), :] = g
            inv[k, tile(t), :] = inverse
        else:
            inverse = jnp.where(upper, 0.0, inverse)
            fwd[k, tile(t), :] = value * inverse
            inv[k, tile(t), :] = inverse
            out[1, tile(slot), :] = jnp.where(upper, pivot, v * (1.0 - g))
            g = jnp.where(upper, 1.0, g)
            gain[k, tile(t), :] = g
            out[0, tile(slot), :] = g * value
    edge = (lanes((SUB, LANE)) == LANE - 1) & (py == places[1] - 1)
    for k in range(depth):
        part = e[COL][k, tile(t), cols - LANE : cols]
        e[COL][k, tile(t), cols - LANE : cols] = jnp.where(edge, 0.0, part)


def close_rows(depth, rows, places, e):
    _, px, _ = position()
    end = slice(rows - SUB, rows)
    for k in range(depth):
        row = e[ROW][k, end, :]
        edge = (sublanes(row.shape) == SUB - 1) & (px == places[0] - 1)
        e[ROW][k, end, :] = jnp.where(edge, 0.0, row)


def inner_kernel(depth, rows, cols, places, low, high, held, *refs):
    both, e, (fwd, gain, inv, out) = refs[FIELDS + held], refs[-9:-4], refs[-4:]
    keep = kept_columns(places[1])

    def unpack(t, carry):
        unpack_columns(depth, cols, keep, t, both, e)
        return carry

    def body(t, carry):
        eliminate(depth, rows, cols, places, t, e, fwd, gain, inv, out, t - low)
        return carry

    sweep(low, min(high, rows // SUB - 1), 2, each(unpack))
    sweep(low, high, INNER, each(body))


def outer_kernel(depth, rows, cols, places, *refs):
    from_above, from_below = refs[8:10]
    e, (fwd, gain, inv, out) = refs[10:15], refs[15:19]
    _, px, _ = position()
    sub = sublanes((SUB, cols + LANE))
    top = (sub >= SUB - 2) & (px > 0)
    low = (sub < 2) & (px < places[0] - 1)
    for f in range(FIELDS):
        for k in range(depth):
            q = f * depth + k
            i = q % 4
            m = (q // 4) * SUB
            above = pltpu.roll(from_above[m : m + SUB, :], (SUB - 2 - 2 * i) % SUB, 0)
            under = pltpu.roll(from_below[m : m + SUB, :], (SUB - 2 * i) % SUB, 0)
            fill = 1.0 if f == GROUND else 0.0
            e[f][k, rows : rows + SUB, :] = jnp.where(top, above, jnp.where(low, under, fill))

    eliminate(depth, rows, cols, places, 0, e, fwd, gain, inv, out, 0)
    eliminate(depth, rows, cols, places, rows // SUB, e, fwd, gain, inv, out, 1)
    close_rows(depth, rows, places, e)


def back(depth, t, fwd, gain, middle, out):
    value = middle
    for k in range(depth - 1, -1, -1):
        value = fwd[k, tile(t), :] + gain[k, tile(t), :] * value
        out[k, tile(t), :] = value


def stencil(k, t, n, count, sub, field, row, col):
    wrap = lambda i: i % count if isinstance(i, int) else i
    z = [field[k, tile(wrap(t + i)), :] for i in range(-1, n + 1)]
    r = [row[k, tile(wrap(t + i)), :] for i in range(-1, n)]
    flows = [a * b for a, b in zip(r, z)]
    totals = []
    for i in range(1, n + 1):
        here = z[i]
        c = col[k, tile(wrap(t + i - 1)), :]
        down = pltpu.roll(jnp.where(sub == 0, z[i + 1], here), SUB - 1, 0)
        up = pltpu.roll(jnp.where(sub == SUB - 1, flows[i - 1], flows[i]), 1, 0)
        across = pltpu.roll(here, here.shape[1] - 1, 1)
        totals.append(r[i] * down + up + c * across + pltpu.roll(c * here, 1, 1))
    return totals, z[1 : n + 1]


def join(depth, t, slot, fwd, gain, mine, theirs, inv4, z):
    ratio = 1.0 / (mine[1, tile(slot), :] + theirs[1, tile(slot), :])
    inv4[tile(t), :] = ratio
    back(depth, t, fwd, gain, (mine[0, tile(slot), :] + theirs[0, tile(slot), :]) * ratio, z)


def image_of(depth, t, n, count, sub, slots, refs):
    right, row, col, via, gain, inv, z, w, fwd2, out = refs
    wrap = lambda i: i % count if isinstance(i, int) else i
    f = [None] * n
    for k in range(depth):
        totals, _ = stencil(k, t, n, count, sub, z, row, col)
        for i in range(n):
            at = tile(wrap(t + i))
            value = right[k, at, :] - totals[i]
            w[k, at, :] = value
            if k:
                value = value + via[k - 1, at, :] * f[i]
            f[i] = value * inv[k, at, :]
            fwd2[k, at, :] = f[i]
            if k == depth - 1:
                out[tile(slots + i), :] = gain[k, at, :] * value


def inner_image_kernel(depth, rows, cols, low, high, first, *refs):
    right, row, col, via, fwd, gain, inv, mine, theirs = refs[0:9]
    z, inv4, w, fwd2, out = refs[-5:]
    count = rows // SUB + 1
    sub = sublanes((SUB, cols + LANE))

    def solve(t):
        join(depth, t, t - low, fwd, gain, mine, theirs, inv4, z)

    begin = low + 1 if first else low - 1
    for t in range(low, begin + 1):
        solve(t)

    def body(t, n, carry):
        for i in range(n):
            solve(t + 1 + i)
        image_of(
            depth, t, n, count, sub, t - 2, (right, row, col, via, gain, inv, z, w, fwd2, out)
        )
        return carry

    sweep(begin, high - 1, IMAGE, body)


def outer_image_kernel(depth, rows, cols, *refs):
    (right, row, col, via, fwd, gain, inv, mine, theirs) = refs[0:9]
    early, (z, inv4, w, fwd2, out, acc) = refs[9], refs[14:20]
    count = rows // SUB + 1
    sub = sublanes((SUB, cols + LANE))
    join(depth, 0, 0, fwd, gain, mine, theirs, inv4, z)
    join(depth, count - 1, 1, fwd, gain, mine, theirs, inv4, z)
    image_of(
        depth, count - 2, 4, count, sub, 0, (right, row, col, via, gain, inv, z, w, fwd2, out)
    )
    carry = (early[0], early[1])
    for t in (count - 2, 0, 1):
        carry = first_dots(depth, cols, t, (right, z, w), carry)
    acc[0], acc[1] = carry


def gathered(sums, parts):
    lane = lanes(sums.shape)
    result = jnp.zeros(sums.shape, jnp.float32)
    for i, part in enumerate(parts):
        total = jnp.sum(jnp.sum(part, axis=0, keepdims=True), axis=1, keepdims=True)
        result = jnp.where(lane == i, total, result)
    return result


def first_dots(depth, cols, t, refs, carry):
    right, z, w = refs
    rho, c = carry
    for k in range(depth):
        zz = z[k, tile(t), 0:cols]
        rho = rho + right[k, tile(t), 0:cols] * zz
        c = c + zz * w[k, tile(t), 0:cols]
    return (rho, c)


def early_kernel(depth, rows, cols, *refs):
    *refs, acc = refs
    zero = jnp.zeros((SUB, cols), jnp.float32)
    body = lambda t, carry: first_dots(depth, cols, t, refs, carry)
    acc[0], acc[1] = sweep(2, rows // SUB - 1, 2, each(body), (zero, zero))


def second_image_of(depth, cols, t, n, count, sub, refs, carry):
    row, col, w, y, v = refs
    e, g = carry
    for k in range(depth):
        totals, fields = stencil(k, t, n, count, sub, y, row, col)
        for i in range(n):
            yy = fields[i][:, 0:cols]
            first = w[k, tile(t + i), 0:cols]
            second = first - totals[i][:, 0:cols]
            v[k, tile(t + i), :] = second
            e = e + first * yy
            g = g + yy * second
    return e, g


def inner_dots_kernel(depth, rows, cols, *refs):
    (row, col, fwd2, gain, mine, theirs, inv4, w, y, v, acc) = refs
    count = rows // SUB + 1
    sub = sublanes((SUB, cols + LANE))

    def solve(t):
        middle = (mine[tile(t - 2), :] + theirs[tile(t - 2), :]) * inv4[tile(t), :]
        back(depth, t, fwd2, gain, middle, y)

    solve(2)
    solve(3)

    def body(t, n, carry):
        for i in range(n):
            solve(t + 1 + i)
        return second_image_of(depth, cols, t, n, count, sub, (row, col, w, y, v), carry)

    zero = jnp.zeros((SUB, cols), jnp.float32)
    acc[0], acc[1] = sweep(3, count - 3, DOTS, body, (zero, zero))


def outer_dots_kernel(depth, rows, cols, *refs):
    (row, col, fwd2, gain, mine, theirs, inv4, w, early, acc) = refs[0:10]
    y, v, sums = refs[12:15]
    count = rows // SUB + 1
    sub = sublanes((SUB, cols + LANE))
    for slot, t in enumerate((count - 2, count - 1, 0, 1)):
        middle = (mine[tile(slot), :] + theirs[tile(slot), :]) * inv4[tile(t), :]
        back(depth, t, fwd2, gain, middle, y)
    carry = (acc[0], acc[1])
    for t, n in ((count - 3, 2), (0, 3)):
        carry = second_image_of(depth, cols, t, n, count, sub, (row, col, w, y, v), carry)
    sums[...] = gathered(sums, (early[0], early[1], *carry))


def final_kernel(depth, rows, cols, *refs):
    (sums, right, z, w, y, v, x_out, r_out, x, r, sem) = refs
    core, _, _ = position()
    total = jnp.sum(sums[...], axis=0, keepdims=True)
    lane = lanes(total.shape)
    rho, c, e, g = (
        jnp.sum(jnp.where(lane == i, total, 0.0), axis=1, keepdims=True) for i in range(4)
    )
    alpha = rho / c
    rho1 = alpha * (alpha * e - c)
    beta = rho1 / rho
    curvature = c - 2.0 * alpha * e + alpha * alpha * g
    alpha1 = rho1 / (curvature - beta * rho1 / alpha)
    near = jnp.broadcast_to(alpha + alpha1 * (1.0 + beta), (SUB, cols))
    far = jnp.broadcast_to(alpha1 * alpha, (SUB, cols))
    copies = []
    for k in range(depth):

        def body(t, carry, k=k):
            x[k, tile(t), :] = near * z[k, tile(t), 0:cols] - far * y[k, tile(t), 0:cols]
            r[k, tile(t), :] = (
                right[k, tile(t), 0:cols] - near * w[k, tile(t), 0:cols] + far * v[k, tile(t), :]
            )
            return carry

        sweep(0, rows // SUB, FINAL, each(body))
        at = layer_of(core, k, depth)
        for slot, (value, target) in enumerate(((x, x_out), (r, r_out))):
            copy = pltpu.make_async_copy(value.at[k], target.at[at], sem.at[slot, k])
            copy.start()
            copies.append(copy)
    for copy in copies:
        copy.wait()


def shift(value, axis, by):
    count = lax.axis_size(axis)
    return lax.ppermute(value, axis, [(i, (i + by) % count) for i in range(count)])


def shards(right_side, row_conduct, column_conduct, via_conduct, via_mask, ground_conduct):
    depth, rows, cols = right_side.shape
    places = (lax.axis_size(PX), lax.axis_size("py"))
    devices = lax.axis_size(ALL)
    tall, wide = rows + SUB, cols + LANE
    ext = (depth, tall, wide)
    vmem, hbm = pltpu.VMEM, pltpu.HBM
    size = depth * tall * wide
    part = functools.partial

    inputs = [right_side, row_conduct, column_conduct, via_conduct, ground_conduct, via_mask]
    strips = (FIELDS * depth * 2, LANE)
    *e, msg_right, msg_left = call(
        part(load_kernel, depth, rows, cols),
        inputs,
        [hbm] * 6,
        [ext] * FIELDS + [strips] * 2,
        [
            pltpu.VMEM((depth, rows, 2 * LANE), jnp.int32),
            pltpu.VMEM((2, rows, LANE), jnp.float32),
            pltpu.SemaphoreType.DMA((3, 6, depth)),
        ],
        flops=size,
        moved=6 * size,
    )
    from_left = shift(msg_right, "py", 1)
    from_right = shift(msg_left, "py", -1)
    e = call(
        part(middle_kernel, depth, rows, cols),
        [*inputs, *e],
        [hbm] * 6 + [vmem] * FIELDS,
        [ext] * FIELDS,
        [
            pltpu.VMEM((depth, rows, cols - 2 * LANE), jnp.int32),
            pltpu.SemaphoreType.DMA((1, 6, depth)),
        ],
        alias={6 + i: i for i in range(FIELDS)},
        flops=10 * size,
        moved=18 * size,
    )
    strips = (FIELDS * depth * 2, wide)
    *e, msg_down, msg_up, both = call(
        part(column_kernel, depth, rows, cols, places[1]),
        [*e, from_left, from_right],
        [vmem] * 7,
        [ext] * FIELDS + [strips] * 2 + [(rows, LANE)],
        alias={i: i for i in range(FIELDS)},
        flops=size,
    )
    from_above = shift(msg_down, PX, 1)
    from_below = shift(msg_up, PX, -1)
    end = rows // SUB
    split = end // 2 + 1
    flops = 15 * size
    *state, mine = call(
        part(inner_kernel, depth, rows, cols, places, 1, split, 0),
        [*e, both],
        [vmem] * 6,
        [ext] * FIELDS + [ext] * 3 + [(2, (split - 1) * SUB, wide)],
        alias={i: i for i in range(FIELDS)},
        flops=flops,
    )
    theirs = shift(mine, "layer", 1)
    *state, mine_rest = call(
        part(inner_kernel, depth, rows, cols, places, split, end, 3),
        [*state, both],
        [vmem] * 9,
        [ext] * FIELDS + [ext] * 3 + [(2, (end - split) * SUB, wide)],
        alias={i: i for i in range(FIELDS + 3)},
        flops=flops,
    )
    theirs_rest = shift(mine_rest, "layer", 1)
    right, row, col, via, _, fwd, gain, inv = state
    images = [ext, (tall, wide), ext, ext, (tall - 4 * SUB, wide)]
    images = call(
        part(inner_image_kernel, depth, rows, cols, 1, split, True),
        [right, row, col, via, fwd, gain, inv, mine, theirs],
        [vmem] * 9,
        images,
        flops=flops,
    )
    z, inv4, w, fwd2, mine2 = call(
        part(inner_image_kernel, depth, rows, cols, split, end, False),
        [right, row, col, via, fwd, gain, inv, mine_rest, theirs_rest, *images],
        [vmem] * 14,
        [ext, (tall, wide), ext, ext, (tall - 4 * SUB, wide)],
        alias={9 + i: i for i in range(5)},
        flops=flops,
    )
    *e, fwd, gain, inv, mine_outer = call(
        part(outer_kernel, depth, rows, cols, places),
        [*state, from_above, from_below],
        [vmem] * 10,
        [ext] * FIELDS + [ext] * 3 + [(2, 2 * SUB, wide)],
        alias={i: i for i in range(FIELDS + 3)},
        flops=3 * size,
    )
    right, row, col, via, _ = e
    theirs_outer = shift(mine_outer, "layer", 1)
    theirs2 = shift(mine2, "layer", 1)
    (early,) = call(
        part(early_kernel, depth, rows, cols),
        [right, z, w],
        [vmem] * 3,
        [(2, SUB, cols)],
        flops=4 * size,
    )
    z, inv4, w, fwd2, mine2_outer, early = call(
        part(outer_image_kernel, depth, rows, cols),
        [right, row, col, via, fwd, gain, inv, mine_outer, theirs_outer, early, z, inv4, w, fwd2],
        [vmem] * 14,
        [ext, (tall, wide), ext, ext, (4 * SUB, wide), (2, SUB, cols)],
        alias={10: 0, 11: 1, 12: 2, 13: 3},
        flops=8 * size,
    )
    theirs2_outer = shift(mine2_outer, "layer", 1)
    block = (depth, rows, cols)
    y, v, acc = call(
        part(inner_dots_kernel, depth, rows, cols),
        [row, col, fwd2, gain, mine2, theirs2, inv4, w],
        [vmem] * 8,
        [ext, block, (2, SUB, cols)],
        flops=20 * size,
    )
    y, v, sums = call(
        part(outer_dots_kernel, depth, rows, cols),
        [row, col, fwd2, gain, mine2_outer, theirs2_outer, inv4, w, early, acc, y, v],
        [vmem] * 12,
        [ext, block, (devices, LANE)],
        alias={10: 0, 11: 1},
        flops=8 * size,
    )
    sums = lax.all_to_all(sums.reshape(devices, 1, LANE), ALL, 0, 0).reshape(devices, LANE)
    result = jax.ShapeDtypeStruct(block, jnp.float32)
    return call(
        part(final_kernel, depth, rows, cols),
        [sums, right, z, w, y, v],
        [vmem] * 6,
        [result] * 2,
        [
            pltpu.VMEM((depth, rows, cols), jnp.float32),
            pltpu.VMEM((depth, rows, cols), jnp.float32),
            pltpu.SemaphoreType.DMA((2, depth)),
        ],
        flops=10 * size,
    )


def solution(mesh):
    count = mesh.shape["px"]
    inner = 4 if count % 4 == 0 else 1
    split = Mesh(
        mesh.devices.reshape(mesh.shape["layer"], count // inner, inner, mesh.shape["py"]),
        ALL,
    )
    spec = P("layer", PX, "py")

    def step(*arrays):
        return tuple(shards(*arrays))

    return jax.shard_map(
        step,
        mesh=split,
        in_specs=(spec,) * 6,
        out_specs=(spec, spec),
        check_vma=False,
    )
```

```python
import functools

import jax
import jax.numpy as jnp
from jax import lax
from jax.experimental import pallas as pl
from jax.experimental.pallas import tpu as pltpu
from jax.sharding import Mesh
from jax.sharding import PartitionSpec as P


RIGHT, ROW, COL, VIA, GROUND = range(5)
FIELDS = 5
EARLY = (RIGHT, ROW)
SUB, LANE = 8, 128
INNER, IMAGE, DOTS, FINAL = 4, 3, 4, 2
TAIL = 3
PX = ("px_0", "px_1")
ALL = ("layer", "px_0", "px_1", "py")


def lanes(shape):
    return lax.broadcasted_iota(jnp.int32, shape, len(shape) - 1)


def sublanes(shape):
    return lax.broadcasted_iota(jnp.int32, shape, len(shape) - 2)


def tile(index):
    if isinstance(index, int):
        return slice(index * SUB, (index + 1) * SUB)
    return pl.ds(pl.multiple_of(index * SUB, SUB), SUB)


def position():
    px = lax.axis_index("px_0") * lax.axis_size("px_1") + lax.axis_index("px_1")
    return (lax.axis_index("layer"), px, lax.axis_index("py"))


def sweep(low, high, several, body, carry=()):
    steps = (high - low) // several
    carry = lax.fori_loop(
        0, steps, lambda i, carry: body(low + i * several, several, carry), carry
    )
    left = high - low - steps * several
    return body(high - left, left, carry) if left else carry


def each(body):
    def run(t, n, carry):
        for i in range(n):
            carry = body(t + i, carry)
        return carry

    return run


def spec_of(kind):
    return pl.BlockSpec(memory_space=kind)


def call(body, operands, kinds, outs, scratch=(), alias=None, flops=0, moved=0, limit=8 << 20):
    shapes = [
        pltpu.VMEM(o, jnp.float32) if isinstance(o, tuple) else o for o in outs
    ]
    operands = [
        pltpu.with_memory_space_constraint(o, k) for o, k in zip(operands, kinds)
    ]
    return pl.pallas_call(
        body,
        out_shape=shapes,
        in_specs=[spec_of(k) for k in kinds],
        out_specs=[spec_of(pltpu.VMEM if isinstance(o, tuple) else pltpu.HBM) for o in outs],
        scratch_shapes=list(scratch),
        input_output_aliases=alias or {},
        compiler_params=pltpu.CompilerParams(vmem_limit_bytes=limit),
        cost_estimate=pl.CostEstimate(flops=flops, bytes_accessed=moved, transcendentals=0),
    )(*operands)


def layer_of(core, k, depth):
    return jnp.where(core == 0, k, depth - 1 - k)


def link_of(core, k, depth):
    upper = depth - 1 if k == depth - 1 else depth - 2 - k
    return jnp.where(core == 0, k, upper)


def start_copies(core, depth, rows, sources, targets, masks, sem, slot, low, high, start, fields):
    copies = []
    for k in range(depth):
        at, link = layer_of(core, k, depth), link_of(core, k, depth)
        for f in fields:
            into = (
                masks.at[k, :, start : start + high - low]
                if f == FIELDS
                else targets[f].at[k, 0:rows, low:high]
            )
            source = sources[f].at[link if f in (VIA, FIELDS) else at, :, low:high]
            copy = pltpu.make_async_copy(source, into, sem.at[slot, f, k])
            copy.start()
            copies.append(copy)
    return copies


def masked(core, depth, layers, t, via, masks, low, high, start):
    for k in layers:
        value = via[k, tile(t), low:high] * masks[k, tile(t), start : start + high - low].astype(
            jnp.float32
        )
        if k == depth - 1:
            value = value * jnp.where(core == 0, 1.0, 0.0).astype(jnp.float32)
        via[k, tile(t), low:high] = value


def load_kernel(depth, rows, cols, *refs):
    sources, e = refs[0:6], refs[6:11]
    msg_right, msg_left, masks, pack, sem = refs[11:]
    core, _, _ = position()
    last = cols - LANE
    begin = functools.partial(start_copies, core, depth, rows, sources, e, masks, sem)
    every = range(FIELDS + 1)
    edges = begin(0, 0, LANE, 0, every) + begin(1, last, cols, LANE, every)
    others = begin(2, LANE, last, 0, EARLY)
    for copy in edges:
        copy.wait()

    def mask(t, carry):
        masked(core, depth, range(depth), t, e[VIA], masks, 0, LANE, 0)
        masked(core, depth, range(depth), t, e[VIA], masks, last, cols, LANE)
        return carry

    sweep(0, rows // SUB, 4, each(mask))
    several = 8 * SUB
    lane = lanes((several, LANE))
    pair = lane // 2

    def place(i, _):
        at = pl.ds(pl.multiple_of(i * several, several), several)
        to_right = to_left = jnp.zeros((several, LANE), jnp.float32)
        for f in range(FIELDS):
            for k in range(depth):
                q = f * depth + k
                tail = e[f][k, at, last:cols]
                head = e[f][k, at, 0:LANE]
                if f == GROUND:
                    across = pltpu.roll(e[COL][k, at, last:cols], 1, 1)
                    tail = tail + jnp.where(lane == LANE - 2, across, 0.0)
                if q:
                    head = pltpu.roll(head, 2 * q, 1)
                to_right = jnp.where(pair == q, pltpu.roll(tail, 2 * q + 2, 1), to_right)
                to_left = jnp.where(pair == q, head, to_left)
        pack[0, at, :] = to_right
        pack[1, at, :] = to_left
        return 0

    lax.fori_loop(0, rows // several, place, 0)
    used = msg_right.shape[0]
    msg_right[...] = pack[0].T[0:used]
    msg_left[...] = pack[1].T[0:used]
    for copy in others:
        copy.wait()


def middle_kernel(depth, rows, cols, *refs):
    sources, e, masks, sem = refs[0:6], refs[11:16], refs[16], refs[17]
    core, _, _ = position()
    low, high = LANE, cols - LANE
    begin = functools.partial(start_copies, core, depth, rows, sources, e, masks, sem, 0, low, high, 0)
    vias = begin((VIA, FIELDS))
    others = begin([f for f in range(FIELDS) if f not in EARLY and f != VIA])
    for k in range(depth):
        for copy in vias[2 * k : 2 * k + 2]:
            copy.wait()

        def body(t, carry, k=k):
            masked(core, depth, (k,), t, e[VIA], masks, low, high, 0)
            return carry

        sweep(0, rows // SUB, 4, each(body))
    for copy in others:
        copy.wait()


def unpack_columns(depth, cols, keep, t, both, e):
    value = both[tile(t), :]
    for f in range(FIELDS):
        for k in range(depth):
            got = pltpu.roll(value, (LANE - (4 * (f * depth + k) + 2)) % LANE, 1)
            fill = 1.0 if f == GROUND else 0.0
            e[f][k, tile(t), cols : cols + LANE] = jnp.where(keep, got, fill)


def kept_columns(places):
    _, _, py = position()
    lane = lanes((SUB, LANE))
    return ((lane < 2) & (py < places - 1)) | ((lane >= LANE - 2) & (py > 0))


def column_kernel(depth, rows, cols, places, *refs):
    from_left, from_right = refs[5:7]
    e = refs[7:12]
    msg_down, msg_up, both = refs[12:15]
    both[...] = jnp.zeros_like(both)
    part = sublanes((SUB, LANE)) // 2
    for m in range(from_left.shape[0] // SUB):
        left = from_left[m * SUB : (m + 1) * SUB, :]
        right = from_right[m * SUB : (m + 1) * SUB, :]
        turn = lambda x, by: pltpu.roll(x, by % SUB, 0) if by % SUB else x
        for half in range(2):
            back_by = -4 * half
            value = jnp.where(part == 0, turn(left, back_by), turn(right, 2 + back_by))
            value = jnp.where(part == 2, turn(left, 2 + back_by), value)
            value = jnp.where(part == 3, turn(right, 4 + back_by), value)
            at = (2 * m + half) * SUB
            both[at : at + SUB, :] = value
    both[...] = both[...].T
    keep = kept_columns(places)
    unpack_columns(depth, cols, keep, 0, both, e)
    unpack_columns(depth, cols, keep, rows // SUB - 1, both, e)
    wide = cols + LANE
    sub = sublanes((SUB, wide))
    end = rows - SUB
    down = up = None
    for f in range(FIELDS):
        for k in range(depth):
            q = f * depth + k
            i = q % 4
            tail = e[f][k, end:rows, :]
            head = e[f][k, 0:SUB, :]
            if f == GROUND:
                across = pltpu.roll(e[ROW][k, end:rows, :], 1, 0)
                tail = tail + jnp.where(sub == SUB - 2, across, 0.0)
            tail = pltpu.roll(tail, (2 * i + 2) % SUB, 0)
            head = pltpu.roll(head, (2 * i) % SUB, 0)
            if i == 0:
                down, up = tail, head
            else:
                down = jnp.where(sub // 2 == i, tail, down)
                up = jnp.where(sub // 2 == i, head, up)
            if i == 3:
                msg_down[(q // 4) * SUB : (q // 4 + 1) * SUB, :] = down
                msg_up[(q // 4) * SUB : (q // 4 + 1) * SUB, :] = up


def eliminate(depth, rows, cols, places, t, e, fwd, gain, inv, out, slot):
    core, _, py = position()
    upper = core == 1
    count = rows // SUB + 1
    sub = sublanes((SUB, cols + LANE))
    before = jnp.where(t == 0, count - 1, t - 1)
    g = f = v = None
    for k in range(depth):
        row = e[ROW][k, tile(t), :]
        col = e[COL][k, tile(t), :]
        row_upper = pltpu.roll(jnp.where(sub == SUB - 1, e[ROW][k, tile(before), :], row), 1, 0)
        pivot = e[GROUND][k, tile(t), :] + row + row_upper + col + pltpu.roll(col, 1, 1)
        value = e[RIGHT][k, tile(t), :]
        if k:
            pivot = pivot + v * (1.0 - g)
            value = value + v * f
        v = e[VIA][k, tile(t), :]
        inverse = 1.0 / (pivot + v)
        g = v * inverse
        if k < depth - 1:
            f = value * inverse
            fwd[k, tile(t), :] = f
            gain[k, tile(t), :] = g
            inv[k, tile(t), :] = inverse
        else:
            inverse = jnp.where(upper, 0.0, inverse)
            fwd[k, tile(t), :] = value * inverse
            inv[k, tile(t), :] = inverse
            out[1, tile(slot), :] = jnp.where(upper, pivot, v * (1.0 - g))
            g = jnp.where(upper, 1.0, g)
            gain[k, tile(t), :] = g
            out[0, tile(slot), :] = g * value
    edge = (lanes((SUB, LANE)) == LANE - 1) & (py == places[1] - 1)
    for k in range(depth):
        part = e[COL][k, tile(t), cols - LANE : cols]
        e[COL][k, tile(t), cols - LANE : cols] = jnp.where(edge, 0.0, part)


def close_rows(depth, rows, places, e):
    _, px, _ = position()
    end = slice(rows - SUB, rows)
    for k in range(depth):
        row = e[ROW][k, end, :]
        edge = (sublanes(row.shape) == SUB - 1) & (px == places[0] - 1)
        e[ROW][k, end, :] = jnp.where(edge, 0.0, row)


def inner_kernel(depth, rows, cols, places, low, high, held, *refs):
    both, e, (fwd, gain, inv, out) = refs[FIELDS + held], refs[-9:-4], refs[-4:]
    keep = kept_columns(places[1])

    def unpack(t, carry):
        unpack_columns(depth, cols, keep, t, both, e)
        return carry

    def body(t, carry):
        eliminate(depth, rows, cols, places, t, e, fwd, gain, inv, out, t - low)
        return carry

    sweep(low, min(high, rows // SUB - 1), 2, each(unpack))
    sweep(low, high, INNER, each(body))


def outer_kernel(depth, rows, cols, places, *refs):
    from_above, from_below = refs[8:10]
    e, (fwd, gain, inv, out) = refs[10:15], refs[15:19]
    _, px, _ = position()
    sub = sublanes((SUB, cols + LANE))
    top = (sub >= SUB - 2) & (px > 0)
    low = (sub < 2) & (px < places[0] - 1)
    for f in range(FIELDS):
        for k in range(depth):
            q = f * depth + k
            i = q % 4
            m = (q // 4) * SUB
            above = pltpu.roll(from_above[m : m + SUB, :], (SUB - 2 - 2 * i) % SUB, 0)
            under = pltpu.roll(from_below[m : m + SUB, :], (SUB - 2 * i) % SUB, 0)
            fill = 1.0 if f == GROUND else 0.0
            e[f][k, rows : rows + SUB, :] = jnp.where(top, above, jnp.where(low, under, fill))

    eliminate(depth, rows, cols, places, 0, e, fwd, gain, inv, out, 0)
    eliminate(depth, rows, cols, places, rows // SUB, e, fwd, gain, inv, out, 1)
    close_rows(depth, rows, places, e)


def back(depth, t, fwd, gain, middle, out):
    value = middle
    for k in range(depth - 1, -1, -1):
        value = fwd[k, tile(t), :] + gain[k, tile(t), :] * value
        out[k, tile(t), :] = value


def stencil(k, t, n, count, sub, field, row, col):
    wrap = lambda i: i % count if isinstance(i, int) else i
    z = [field[k, tile(wrap(t + i)), :] for i in range(-1, n + 1)]
    r = [row[k, tile(wrap(t + i)), :] for i in range(-1, n)]
    flows = [a * b for a, b in zip(r, z)]
    totals = []
    for i in range(1, n + 1):
        here = z[i]
        c = col[k, tile(wrap(t + i - 1)), :]
        down = pltpu.roll(jnp.where(sub == 0, z[i + 1], here), SUB - 1, 0)
        up = pltpu.roll(jnp.where(sub == SUB - 1, flows[i - 1], flows[i]), 1, 0)
        across = pltpu.roll(here, here.shape[1] - 1, 1)
        totals.append(r[i] * down + up + c * across + pltpu.roll(c * here, 1, 1))
    return totals, z[1 : n + 1]


def join(depth, t, slot, fwd, gain, mine, theirs, inv4, z):
    ratio = 1.0 / (mine[1, tile(slot), :] + theirs[1, tile(slot), :])
    inv4[tile(t), :] = ratio
    back(depth, t, fwd, gain, (mine[0, tile(slot), :] + theirs[0, tile(slot), :]) * ratio, z)


def image_of(depth, t, n, count, sub, slots, refs):
    right, row, col, via, gain, inv, z, w, fwd2, out = refs
    wrap = lambda i: i % count if isinstance(i, int) else i
    f = [None] * n
    for k in range(depth):
        totals, _ = stencil(k, t, n, count, sub, z, row, col)
        for i in range(n):
            at = tile(wrap(t + i))
            value = right[k, at, :] - totals[i]
            w[k, at, :] = value
            if k:
                value = value + via[k - 1, at, :] * f[i]
            f[i] = value * inv[k, at, :]
            fwd2[k, at, :] = f[i]
            if k == depth - 1:
                out[tile(slots + i), :] = gain[k, at, :] * value


def inner_image_kernel(depth, rows, cols, low, high, begin, end, *refs):
    right, row, col, via, fwd, gain, inv, mine, theirs = refs[0:9]
    z, inv4, w, fwd2, out = refs[-5:]
    count = rows // SUB + 1
    sub = sublanes((SUB, cols + LANE))

    def solve(t):
        join(depth, t, t - low, fwd, gain, mine, theirs, inv4, z)

    for t in range(low, begin + 1):
        solve(t)

    def body(t, n, carry):
        for i in range(n):
            solve(t + 1 + i)
        image_of(
            depth, t, n, count, sub, t - 2, (right, row, col, via, gain, inv, z, w, fwd2, out)
        )
        return carry

    sweep(begin, end, IMAGE, body)
    for t in range(end + 1, high):
        solve(t)


def outer_image_kernel(depth, rows, cols, *refs):
    (right, row, col, via, fwd, gain, inv, mine, theirs) = refs[0:9]
    early, (z, inv4, w, fwd2, out, acc) = refs[9], refs[15:21]
    count = rows // SUB + 1
    sub = sublanes((SUB, cols + LANE))
    join(depth, 0, 0, fwd, gain, mine, theirs, inv4, z)
    join(depth, count - 1, 1, fwd, gain, mine, theirs, inv4, z)
    image_of(
        depth, count - 2, 4, count, sub, 0, (right, row, col, via, gain, inv, z, w, fwd2, out)
    )
    carry = (early[0], early[1])
    for t in (count - 2, 0, 1):
        carry = first_dots(depth, cols, t, (right, z, w), carry)
    acc[0], acc[1] = carry


def gathered(sums, parts):
    lane = lanes(sums.shape)
    result = jnp.zeros(sums.shape, jnp.float32)
    for i, part in enumerate(parts):
        total = jnp.sum(jnp.sum(part, axis=0, keepdims=True), axis=1, keepdims=True)
        result = jnp.where(lane == i, total, result)
    return result


def first_dots(depth, cols, t, refs, carry):
    right, z, w = refs
    rho, c = carry
    for k in range(depth):
        zz = z[k, tile(t), 0:cols]
        rho = rho + right[k, tile(t), 0:cols] * zz
        c = c + zz * w[k, tile(t), 0:cols]
    return (rho, c)


def tail_kernel(depth, rows, cols, begin, *refs):
    right, row, col, via, gain, inv, z = refs[0:7]
    w, fwd2, out, acc = refs[9:13]
    count = rows // SUB + 1
    sub = sublanes((SUB, cols + LANE))
    image_of(
        depth,
        begin,
        count - 2 - begin,
        count,
        sub,
        4,
        (right, row, col, via, gain, inv, z, w, fwd2, out),
    )
    zero = jnp.zeros((SUB, cols), jnp.float32)
    body = lambda t, carry: first_dots(depth, cols, t, (right, z, w), carry)
    acc[0], acc[1] = sweep(2, rows // SUB - 1, 2, each(body), (zero, zero))


def second_image_of(depth, cols, t, n, count, sub, refs, carry):
    row, col, w, y, v = refs
    e, g = carry
    for k in range(depth):
        totals, fields = stencil(k, t, n, count, sub, y, row, col)
        for i in range(n):
            yy = fields[i][:, 0:cols]
            first = w[k, tile(t + i), 0:cols]
            second = first - totals[i][:, 0:cols]
            v[k, tile(t + i), :] = second
            e = e + first * yy
            g = g + yy * second
    return e, g


def inner_dots_kernel(depth, rows, cols, end, *refs):
    (row, col, fwd2, gain, mine, theirs, inv4, w, y, v, acc) = refs
    count = rows // SUB + 1
    sub = sublanes((SUB, cols + LANE))

    def solve(t):
        middle = (mine[tile(t - 2), :] + theirs[tile(t - 2), :]) * inv4[tile(t), :]
        back(depth, t, fwd2, gain, middle, y)

    solve(2)
    solve(3)

    def body(t, n, carry):
        for i in range(n):
            solve(t + 1 + i)
        return second_image_of(depth, cols, t, n, count, sub, (row, col, w, y, v), carry)

    zero = jnp.zeros((SUB, cols), jnp.float32)
    acc[0], acc[1] = sweep(3, end - 1, DOTS, body, (zero, zero))


def outer_dots_kernel(depth, rows, cols, begin, *refs):
    (row, col, fwd2, gain, mine, theirs, inv4, w, early, acc) = refs[0:10]
    y, v, sums = refs[12:15]
    count = rows // SUB + 1
    sub = sublanes((SUB, cols + LANE))
    for slot, t in enumerate((count - 2, count - 1, 0, 1, *range(begin, count - 2))):
        middle = (mine[tile(slot), :] + theirs[tile(slot), :]) * inv4[tile(t), :]
        back(depth, t, fwd2, gain, middle, y)
    carry = (acc[0], acc[1])
    for t, n in ((begin - 1, count - begin), (0, 3)):
        carry = second_image_of(depth, cols, t, n, count, sub, (row, col, w, y, v), carry)
    sums[...] = gathered(sums, (early[0], early[1], *carry))


def final_kernel(depth, rows, cols, *refs):
    (sums, right, z, w, y, v, x_out, r_out, x, r, sem) = refs
    core, _, _ = position()
    total = jnp.sum(sums[...], axis=0, keepdims=True)
    lane = lanes(total.shape)
    rho, c, e, g = (
        jnp.sum(jnp.where(lane == i, total, 0.0), axis=1, keepdims=True) for i in range(4)
    )
    alpha = rho / c
    rho1 = alpha * (alpha * e - c)
    beta = rho1 / rho
    curvature = c - 2.0 * alpha * e + alpha * alpha * g
    alpha1 = rho1 / (curvature - beta * rho1 / alpha)
    near = jnp.broadcast_to(alpha + alpha1 * (1.0 + beta), (SUB, cols))
    far = jnp.broadcast_to(alpha1 * alpha, (SUB, cols))
    copies = []
    for k in range(depth):

        def body(t, carry, k=k):
            x[k, tile(t), :] = near * z[k, tile(t), 0:cols] - far * y[k, tile(t), 0:cols]
            r[k, tile(t), :] = (
                right[k, tile(t), 0:cols] - near * w[k, tile(t), 0:cols] + far * v[k, tile(t), :]
            )
            return carry

        sweep(0, rows // SUB, FINAL, each(body))
        at = layer_of(core, k, depth)
        for slot, (value, target) in enumerate(((x, x_out), (r, r_out))):
            copy = pltpu.make_async_copy(value.at[k], target.at[at], sem.at[slot, k])
            copy.start()
            copies.append(copy)
    for copy in copies:
        copy.wait()


def shift(value, axis, by):
    count = lax.axis_size(axis)
    return lax.ppermute(value, axis, [(i, (i + by) % count) for i in range(count)])


def shards(right_side, row_conduct, column_conduct, via_conduct, via_mask, ground_conduct):
    depth, rows, cols = right_side.shape
    places = (lax.axis_size(PX), lax.axis_size("py"))
    devices = lax.axis_size(ALL)
    tall, wide = rows + SUB, cols + LANE
    ext = (depth, tall, wide)
    vmem, hbm = pltpu.VMEM, pltpu.HBM
    size = depth * tall * wide
    part = functools.partial

    inputs = [right_side, row_conduct, column_conduct, via_conduct, ground_conduct, via_mask]
    strips = (FIELDS * depth * 2, LANE)
    *e, msg_right, msg_left = call(
        part(load_kernel, depth, rows, cols),
        inputs,
        [hbm] * 6,
        [ext] * FIELDS + [strips] * 2,
        [
            pltpu.VMEM((depth, rows, 2 * LANE), jnp.int32),
            pltpu.VMEM((2, rows, LANE), jnp.float32),
            pltpu.SemaphoreType.DMA((3, 6, depth)),
        ],
        flops=size,
        moved=6 * size,
    )
    from_left = shift(msg_right, "py", 1)
    from_right = shift(msg_left, "py", -1)
    e = call(
        part(middle_kernel, depth, rows, cols),
        [*inputs, *e],
        [hbm] * 6 + [vmem] * FIELDS,
        [ext] * FIELDS,
        [
            pltpu.VMEM((depth, rows, cols - 2 * LANE), jnp.int32),
            pltpu.SemaphoreType.DMA((1, 6, depth)),
        ],
        alias={6 + i: i for i in range(FIELDS)},
        flops=10 * size,
        moved=18 * size,
    )
    strips = (FIELDS * depth * 2, wide)
    *e, msg_down, msg_up, both = call(
        part(column_kernel, depth, rows, cols, places[1]),
        [*e, from_left, from_right],
        [vmem] * 7,
        [ext] * FIELDS + [strips] * 2 + [(rows, LANE)],
        alias={i: i for i in range(FIELDS)},
        flops=size,
    )
    from_above = shift(msg_down, PX, 1)
    from_below = shift(msg_up, PX, -1)
    end = rows // SUB
    split = end // 2 + 1
    flops = 15 * size
    *state, mine = call(
        part(inner_kernel, depth, rows, cols, places, 1, split, 0),
        [*e, both],
        [vmem] * 6,
        [ext] * FIELDS + [ext] * 3 + [(2, (split - 1) * SUB, wide)],
        alias={i: i for i in range(FIELDS)},
        flops=flops,
    )
    theirs = shift(mine, "layer", 1)
    *state, mine_rest = call(
        part(inner_kernel, depth, rows, cols, places, split, end, 3),
        [*state, both],
        [vmem] * 9,
        [ext] * FIELDS + [ext] * 3 + [(2, (end - split) * SUB, wide)],
        alias={i: i for i in range(FIELDS + 3)},
        flops=flops,
    )
    theirs_rest = shift(mine_rest, "layer", 1)
    right, row, col, via, _, fwd, gain, inv = state
    late = end - 1 - TAIL
    images = [ext, (tall, wide), ext, ext, ((late - 2) * SUB, wide)]
    first = call(
        part(inner_image_kernel, depth, rows, cols, 1, split, 2, split - 1),
        [right, row, col, via, fwd, gain, inv, mine, theirs],
        [vmem] * 9,
        images,
        flops=flops,
    )
    z, inv4, w, fwd2, mine2 = call(
        part(inner_image_kernel, depth, rows, cols, split, end, split - 1, late),
        [right, row, col, via, fwd, gain, inv, mine_rest, theirs_rest, *first],
        [vmem] * 14,
        images,
        alias={9 + i: i for i in range(5)},
        flops=flops,
    )
    *e, fwd, gain, inv, mine_outer = call(
        part(outer_kernel, depth, rows, cols, places),
        [*state, from_above, from_below],
        [vmem] * 10,
        [ext] * FIELDS + [ext] * 3 + [(2, 2 * SUB, wide)],
        alias={i: i for i in range(FIELDS + 3)},
        flops=3 * size,
    )
    right, row, col, via, _ = e
    theirs_outer = shift(mine_outer, "layer", 1)
    theirs2 = shift(mine2, "layer", 1)
    w, fwd2, mine2_outer, early = call(
        part(tail_kernel, depth, rows, cols, late),
        [right, row, col, via, gain, inv, z, w, fwd2],
        [vmem] * 9,
        [ext, ext, ((4 + TAIL) * SUB, wide), (2, SUB, cols)],
        alias={7: 0, 8: 1},
        flops=8 * size,
    )
    z, inv4, w, fwd2, mine2_outer, early = call(
        part(outer_image_kernel, depth, rows, cols),
        [right, row, col, via, fwd, gain, inv, mine_outer, theirs_outer, early]
        + [z, inv4, w, fwd2, mine2_outer],
        [vmem] * 15,
        [ext, (tall, wide), ext, ext, ((4 + TAIL) * SUB, wide), (2, SUB, cols)],
        alias={10: 0, 11: 1, 12: 2, 13: 3, 14: 4},
        flops=8 * size,
    )
    theirs2_outer = shift(mine2_outer, "layer", 1)
    block = (depth, rows, cols)
    y, v, acc = call(
        part(inner_dots_kernel, depth, rows, cols, late),
        [row, col, fwd2, gain, mine2, theirs2, inv4, w],
        [vmem] * 8,
        [ext, block, (2, SUB, cols)],
        flops=20 * size,
    )
    y, v, sums = call(
        part(outer_dots_kernel, depth, rows, cols, late),
        [row, col, fwd2, gain, mine2_outer, theirs2_outer, inv4, w, early, acc, y, v],
        [vmem] * 12,
        [ext, block, (devices, LANE)],
        alias={10: 0, 11: 1},
        flops=8 * size,
    )
    sums = lax.all_to_all(sums.reshape(devices, 1, LANE), ALL, 0, 0).reshape(devices, LANE)
    result = jax.ShapeDtypeStruct(block, jnp.float32)
    return call(
        part(final_kernel, depth, rows, cols),
        [sums, right, z, w, y, v],
        [vmem] * 6,
        [result] * 2,
        [
            pltpu.VMEM((depth, rows, cols), jnp.float32),
            pltpu.VMEM((depth, rows, cols), jnp.float32),
            pltpu.SemaphoreType.DMA((2, depth)),
        ],
        flops=10 * size,
    )


def solution(mesh):
    count = mesh.shape["px"]
    inner = 4 if count % 4 == 0 else 1
    split = Mesh(
        mesh.devices.reshape(mesh.shape["layer"], count // inner, inner, mesh.shape["py"]),
        ALL,
    )
    spec = P("layer", PX, "py")

    def step(*arrays):
        return tuple(shards(*arrays))

    return jax.shard_map(
        step,
        mesh=split,
        in_specs=(spec,) * 6,
        out_specs=(spec, spec),
        check_vma=False,
    )
```

```python
import functools

import jax
import jax.numpy as jnp
from jax import lax
from jax.experimental import pallas as pl
from jax.experimental.pallas import tpu as pltpu
from jax.sharding import Mesh
from jax.sharding import PartitionSpec as P


RIGHT, ROW, COL, VIA, GROUND = range(5)
FIELDS = 5
EARLY = (RIGHT, ROW)
SUB, LANE = 8, 128
INNER, IMAGE, DOTS, FINAL = 4, 3, 3, 2
TAIL = 2
PX = ("px_0", "px_1")
ALL = ("layer", "px_0", "px_1", "py")


def lanes(shape):
    return lax.broadcasted_iota(jnp.int32, shape, len(shape) - 1)


def sublanes(shape):
    return lax.broadcasted_iota(jnp.int32, shape, len(shape) - 2)


def tile(index):
    if isinstance(index, int):
        return slice(index * SUB, (index + 1) * SUB)
    return pl.ds(pl.multiple_of(index * SUB, SUB), SUB)


def position():
    px = lax.axis_index("px_0") * lax.axis_size("px_1") + lax.axis_index("px_1")
    return (lax.axis_index("layer"), px, lax.axis_index("py"))


def sweep(low, high, several, body, carry=()):
    steps = (high - low) // several
    carry = lax.fori_loop(
        0, steps, lambda i, carry: body(low + i * several, several, carry), carry
    )
    left = high - low - steps * several
    return body(high - left, left, carry) if left else carry


def each(body):
    def run(t, n, carry):
        for i in range(n):
            carry = body(t + i, carry)
        return carry

    return run


def spec_of(kind):
    return pl.BlockSpec(memory_space=kind)


def call(body, operands, kinds, outs, scratch=(), alias=None, flops=0, moved=0, limit=8 << 20):
    shapes = [
        pltpu.VMEM(o, jnp.float32) if isinstance(o, tuple) else o for o in outs
    ]
    operands = [
        pltpu.with_memory_space_constraint(o, k) for o, k in zip(operands, kinds)
    ]
    return pl.pallas_call(
        body,
        out_shape=shapes,
        in_specs=[spec_of(k) for k in kinds],
        out_specs=[spec_of(pltpu.VMEM if isinstance(o, tuple) else pltpu.HBM) for o in outs],
        scratch_shapes=list(scratch),
        input_output_aliases=alias or {},
        compiler_params=pltpu.CompilerParams(vmem_limit_bytes=limit),
        cost_estimate=pl.CostEstimate(flops=flops, bytes_accessed=moved, transcendentals=0),
    )(*operands)


def layer_of(core, k, depth):
    return jnp.where(core == 0, k, depth - 1 - k)


def link_of(core, k, depth):
    upper = depth - 1 if k == depth - 1 else depth - 2 - k
    return jnp.where(core == 0, k, upper)


def start_copies(core, depth, rows, sources, targets, masks, sem, slot, low, high, start, fields):
    copies = []
    for k in range(depth):
        at, link = layer_of(core, k, depth), link_of(core, k, depth)
        for f in fields:
            into = (
                masks.at[k, :, start : start + high - low]
                if f == FIELDS
                else targets[f].at[k, 0:rows, low:high]
            )
            source = sources[f].at[link if f in (VIA, FIELDS) else at, :, low:high]
            copy = pltpu.make_async_copy(source, into, sem.at[slot, f, k])
            copy.start()
            copies.append(copy)
    return copies


def masked(core, depth, layers, t, via, masks, low, high, start):
    for k in layers:
        value = via[k, tile(t), low:high] * masks[k, tile(t), start : start + high - low].astype(
            jnp.float32
        )
        if k == depth - 1:
            value = value * jnp.where(core == 0, 1.0, 0.0).astype(jnp.float32)
        via[k, tile(t), low:high] = value


def load_kernel(depth, rows, cols, *refs):
    sources, e = refs[0:6], refs[6:11]
    msg_right, msg_left, masks, pack, sem = refs[11:]
    core, _, _ = position()
    last = cols - LANE
    begin = functools.partial(start_copies, core, depth, rows, sources, e, masks, sem)
    every = range(FIELDS + 1)
    edges = begin(0, 0, LANE, 0, every) + begin(1, last, cols, LANE, every)
    others = begin(2, LANE, last, 0, EARLY)
    for copy in edges:
        copy.wait()

    def mask(t, carry):
        masked(core, depth, range(depth), t, e[VIA], masks, 0, LANE, 0)
        masked(core, depth, range(depth), t, e[VIA], masks, last, cols, LANE)
        return carry

    sweep(0, rows // SUB, 4, each(mask))
    several = 8 * SUB
    lane = lanes((several, LANE))
    pair = lane // 2

    def place(i, _):
        at = pl.ds(pl.multiple_of(i * several, several), several)
        to_right = to_left = jnp.zeros((several, LANE), jnp.float32)
        for f in range(FIELDS):
            for k in range(depth):
                q = f * depth + k
                tail = e[f][k, at, last:cols]
                head = e[f][k, at, 0:LANE]
                if f == GROUND:
                    across = pltpu.roll(e[COL][k, at, last:cols], 1, 1)
                    tail = tail + jnp.where(lane == LANE - 2, across, 0.0)
                if q:
                    head = pltpu.roll(head, 2 * q, 1)
                to_right = jnp.where(pair == q, pltpu.roll(tail, 2 * q + 2, 1), to_right)
                to_left = jnp.where(pair == q, head, to_left)
        pack[0, at, :] = to_right
        pack[1, at, :] = to_left
        return 0

    lax.fori_loop(0, rows // several, place, 0)
    used = msg_right.shape[0]
    msg_right[...] = pack[0].T[0:used]
    msg_left[...] = pack[1].T[0:used]
    for copy in others:
        copy.wait()


def middle_kernel(depth, rows, cols, *refs):
    sources, e, masks, sem = refs[0:6], refs[11:16], refs[16], refs[17]
    core, _, _ = position()
    low, high = LANE, cols - LANE
    begin = functools.partial(start_copies, core, depth, rows, sources, e, masks, sem, 0, low, high, 0)
    vias = begin((VIA, FIELDS))
    others = begin([f for f in range(FIELDS) if f not in EARLY and f != VIA])
    for k in range(depth):
        for copy in vias[2 * k : 2 * k + 2]:
            copy.wait()

        def body(t, carry, k=k):
            masked(core, depth, (k,), t, e[VIA], masks, low, high, 0)
            return carry

        sweep(0, rows // SUB, 4, each(body))
    for copy in others:
        copy.wait()


def unpack_columns(depth, cols, keep, t, both, e):
    value = both[tile(t), :]
    for f in range(FIELDS):
        for k in range(depth):
            got = pltpu.roll(value, (LANE - (4 * (f * depth + k) + 2)) % LANE, 1)
            fill = 1.0 if f == GROUND else 0.0
            e[f][k, tile(t), cols : cols + LANE] = jnp.where(keep, got, fill)


def kept_columns(places):
    _, _, py = position()
    lane = lanes((SUB, LANE))
    return ((lane < 2) & (py < places - 1)) | ((lane >= LANE - 2) & (py > 0))


def column_kernel(depth, rows, cols, places, *refs):
    from_left, from_right = refs[5:7]
    e = refs[7:12]
    msg_down, msg_up, both = refs[12:15]
    both[...] = jnp.zeros_like(both)
    part = sublanes((SUB, LANE)) // 2
    for m in range(from_left.shape[0] // SUB):
        left = from_left[m * SUB : (m + 1) * SUB, :]
        right = from_right[m * SUB : (m + 1) * SUB, :]
        turn = lambda x, by: pltpu.roll(x, by % SUB, 0) if by % SUB else x
        for half in range(2):
            back_by = -4 * half
            value = jnp.where(part == 0, turn(left, back_by), turn(right, 2 + back_by))
            value = jnp.where(part == 2, turn(left, 2 + back_by), value)
            value = jnp.where(part == 3, turn(right, 4 + back_by), value)
            at = (2 * m + half) * SUB
            both[at : at + SUB, :] = value
    both[...] = both[...].T
    keep = kept_columns(places)
    unpack_columns(depth, cols, keep, 0, both, e)
    unpack_columns(depth, cols, keep, rows // SUB - 1, both, e)
    wide = cols + LANE
    sub = sublanes((SUB, wide))
    end = rows - SUB
    down = up = None
    for f in range(FIELDS):
        for k in range(depth):
            q = f * depth + k
            i = q % 4
            tail = e[f][k, end:rows, :]
            head = e[f][k, 0:SUB, :]
            if f == GROUND:
                across = pltpu.roll(e[ROW][k, end:rows, :], 1, 0)
                tail = tail + jnp.where(sub == SUB - 2, across, 0.0)
            tail = pltpu.roll(tail, (2 * i + 2) % SUB, 0)
            head = pltpu.roll(head, (2 * i) % SUB, 0)
            if i == 0:
                down, up = tail, head
            else:
                down = jnp.where(sub // 2 == i, tail, down)
                up = jnp.where(sub // 2 == i, head, up)
            if i == 3:
                msg_down[(q // 4) * SUB : (q // 4 + 1) * SUB, :] = down
                msg_up[(q // 4) * SUB : (q // 4 + 1) * SUB, :] = up


def eliminate(depth, rows, cols, places, t, e, fwd, gain, inv, out, slot):
    core, _, py = position()
    upper = core == 1
    count = rows // SUB + 1
    sub = sublanes((SUB, cols + LANE))
    before = jnp.where(t == 0, count - 1, t - 1)
    g = f = v = None
    for k in range(depth):
        row = e[ROW][k, tile(t), :]
        col = e[COL][k, tile(t), :]
        row_upper = pltpu.roll(jnp.where(sub == SUB - 1, e[ROW][k, tile(before), :], row), 1, 0)
        pivot = e[GROUND][k, tile(t), :] + row + row_upper + col + pltpu.roll(col, 1, 1)
        value = e[RIGHT][k, tile(t), :]
        if k:
            pivot = pivot + v * (1.0 - g)
            value = value + v * f
        v = e[VIA][k, tile(t), :]
        inverse = 1.0 / (pivot + v)
        g = v * inverse
        if k < depth - 1:
            f = value * inverse
            fwd[k, tile(t), :] = f
            gain[k, tile(t), :] = g
            inv[k, tile(t), :] = inverse
        else:
            inverse = jnp.where(upper, 0.0, inverse)
            fwd[k, tile(t), :] = value * inverse
            inv[k, tile(t), :] = inverse
            out[1, tile(slot), :] = jnp.where(upper, pivot, v * (1.0 - g))
            g = jnp.where(upper, 1.0, g)
            gain[k, tile(t), :] = g
            out[0, tile(slot), :] = g * value
    edge = (lanes((SUB, LANE)) == LANE - 1) & (py == places[1] - 1)
    for k in range(depth):
        part = e[COL][k, tile(t), cols - LANE : cols]
        e[COL][k, tile(t), cols - LANE : cols] = jnp.where(edge, 0.0, part)


def close_rows(depth, rows, places, e):
    _, px, _ = position()
    end = slice(rows - SUB, rows)
    for k in range(depth):
        row = e[ROW][k, end, :]
        edge = (sublanes(row.shape) == SUB - 1) & (px == places[0] - 1)
        e[ROW][k, end, :] = jnp.where(edge, 0.0, row)


def inner_kernel(depth, rows, cols, places, low, high, held, *refs):
    both, e, (fwd, gain, inv, out) = refs[FIELDS + held], refs[-9:-4], refs[-4:]
    keep = kept_columns(places[1])

    def unpack(t, carry):
        unpack_columns(depth, cols, keep, t, both, e)
        return carry

    def body(t, carry):
        eliminate(depth, rows, cols, places, t, e, fwd, gain, inv, out, t - low)
        return carry

    sweep(low, min(high, rows // SUB - 1), 2, each(unpack))
    sweep(low, high, INNER, each(body))


def outer_kernel(depth, rows, cols, places, *refs):
    from_above, from_below = refs[8:10]
    e, (fwd, gain, inv, out) = refs[10:15], refs[15:19]
    _, px, _ = position()
    sub = sublanes((SUB, cols + LANE))
    top = (sub >= SUB - 2) & (px > 0)
    low = (sub < 2) & (px < places[0] - 1)
    for f in range(FIELDS):
        for k in range(depth):
            q = f * depth + k
            i = q % 4
            m = (q // 4) * SUB
            above = pltpu.roll(from_above[m : m + SUB, :], (SUB - 2 - 2 * i) % SUB, 0)
            under = pltpu.roll(from_below[m : m + SUB, :], (SUB - 2 * i) % SUB, 0)
            fill = 1.0 if f == GROUND else 0.0
            e[f][k, rows : rows + SUB, :] = jnp.where(top, above, jnp.where(low, under, fill))

    eliminate(depth, rows, cols, places, 0, e, fwd, gain, inv, out, 0)
    eliminate(depth, rows, cols, places, rows // SUB, e, fwd, gain, inv, out, 1)
    close_rows(depth, rows, places, e)


def back(depth, t, fwd, gain, middle, out):
    value = middle
    for k in range(depth - 1, -1, -1):
        value = fwd[k, tile(t), :] + gain[k, tile(t), :] * value
        out[k, tile(t), :] = value


def stencil(k, t, n, count, sub, field, row, col):
    wrap = lambda i: i % count if isinstance(i, int) else i
    z = [field[k, tile(wrap(t + i)), :] for i in range(-1, n + 1)]
    r = [row[k, tile(wrap(t + i)), :] for i in range(-1, n)]
    flows = [a * b for a, b in zip(r, z)]
    totals = []
    for i in range(1, n + 1):
        here = z[i]
        c = col[k, tile(wrap(t + i - 1)), :]
        down = pltpu.roll(jnp.where(sub == 0, z[i + 1], here), SUB - 1, 0)
        up = pltpu.roll(jnp.where(sub == SUB - 1, flows[i - 1], flows[i]), 1, 0)
        across = pltpu.roll(here, here.shape[1] - 1, 1)
        totals.append(r[i] * down + up + c * across + pltpu.roll(c * here, 1, 1))
    return totals, z[1 : n + 1]


def join(depth, t, slot, fwd, gain, mine, theirs, inv4, z):
    ratio = 1.0 / (mine[1, tile(slot), :] + theirs[1, tile(slot), :])
    inv4[tile(t), :] = ratio
    back(depth, t, fwd, gain, (mine[0, tile(slot), :] + theirs[0, tile(slot), :]) * ratio, z)


def image_of(depth, t, n, count, sub, slots, refs):
    right, row, col, via, gain, inv, z, w, fwd2, out = refs
    wrap = lambda i: i % count if isinstance(i, int) else i
    f = [None] * n
    for k in range(depth):
        totals, _ = stencil(k, t, n, count, sub, z, row, col)
        for i in range(n):
            at = tile(wrap(t + i))
            value = right[k, at, :] - totals[i]
            w[k, at, :] = value
            if k:
                value = value + via[k - 1, at, :] * f[i]
            f[i] = value * inv[k, at, :]
            fwd2[k, at, :] = f[i]
            if k == depth - 1:
                out[tile(slots + i), :] = gain[k, at, :] * value


def inner_image_kernel(depth, rows, cols, low, high, begin, end, *refs):
    right, row, col, via, fwd, gain, inv, mine, theirs = refs[0:9]
    z, inv4, w, fwd2, out = refs[-5:]
    count = rows // SUB + 1
    sub = sublanes((SUB, cols + LANE))

    def solve(t):
        join(depth, t, t - low, fwd, gain, mine, theirs, inv4, z)

    for t in range(low, begin + 1):
        solve(t)

    def body(t, n, carry):
        for i in range(n):
            solve(t + 1 + i)
        image_of(
            depth, t, n, count, sub, t - 2, (right, row, col, via, gain, inv, z, w, fwd2, out)
        )
        return carry

    sweep(begin, end, IMAGE, body)
    for t in range(end + 1, high):
        solve(t)


def outer_image_kernel(depth, rows, cols, *refs):
    (right, row, col, via, fwd, gain, inv, mine, theirs) = refs[0:9]
    early, (z, inv4, w, fwd2, out, acc) = refs[9], refs[15:21]
    count = rows // SUB + 1
    sub = sublanes((SUB, cols + LANE))
    join(depth, 0, 0, fwd, gain, mine, theirs, inv4, z)
    join(depth, count - 1, 1, fwd, gain, mine, theirs, inv4, z)
    image_of(
        depth, count - 2, 4, count, sub, 0, (right, row, col, via, gain, inv, z, w, fwd2, out)
    )
    carry = (early[0], early[1])
    for t in (count - 2, 0, 1):
        carry = first_dots(depth, cols, t, (right, z, w), carry)
    acc[0], acc[1] = carry


def gathered(sums, parts):
    lane = lanes(sums.shape)
    result = jnp.zeros(sums.shape, jnp.float32)
    for i, part in enumerate(parts):
        total = jnp.sum(jnp.sum(part, axis=0, keepdims=True), axis=1, keepdims=True)
        result = jnp.where(lane == i, total, result)
    return result


def first_dots(depth, cols, t, refs, carry):
    right, z, w = refs
    rho, c = carry
    for k in range(depth):
        zz = z[k, tile(t), 0:cols]
        rho = rho + right[k, tile(t), 0:cols] * zz
        c = c + zz * w[k, tile(t), 0:cols]
    return (rho, c)


def tail_kernel(depth, rows, cols, begin, *refs):
    right, row, col, via, gain, inv, z = refs[0:7]
    w, fwd2, out, acc = refs[9:13]
    count = rows // SUB + 1
    sub = sublanes((SUB, cols + LANE))
    image_of(
        depth,
        begin,
        count - 2 - begin,
        count,
        sub,
        4,
        (right, row, col, via, gain, inv, z, w, fwd2, out),
    )
    zero = jnp.zeros((SUB, cols), jnp.float32)
    body = lambda t, carry: first_dots(depth, cols, t, (right, z, w), carry)
    acc[0], acc[1] = sweep(2, rows // SUB - 1, 2, each(body), (zero, zero))


def second_image_of(depth, cols, t, n, count, sub, refs, carry):
    row, col, w, y, v = refs
    e, g = carry
    for k in range(depth):
        totals, fields = stencil(k, t, n, count, sub, y, row, col)
        for i in range(n):
            yy = fields[i][:, 0:cols]
            first = w[k, tile(t + i), 0:cols]
            second = first - totals[i][:, 0:cols]
            v[k, tile(t + i), :] = second
            e = e + first * yy
            g = g + yy * second
    return e, g


def inner_dots_kernel(depth, rows, cols, end, *refs):
    (row, col, fwd2, gain, mine, theirs, inv4, w, y, v, acc) = refs
    count = rows // SUB + 1
    sub = sublanes((SUB, cols + LANE))

    def solve(t):
        middle = (mine[tile(t - 2), :] + theirs[tile(t - 2), :]) * inv4[tile(t), :]
        back(depth, t, fwd2, gain, middle, y)

    solve(2)
    solve(3)

    def body(t, n, carry):
        for i in range(n):
            solve(t + 1 + i)
        return second_image_of(depth, cols, t, n, count, sub, (row, col, w, y, v), carry)

    zero = jnp.zeros((SUB, cols), jnp.float32)
    acc[0], acc[1] = sweep(3, end - 1, DOTS, body, (zero, zero))


def outer_dots_kernel(depth, rows, cols, begin, *refs):
    (row, col, fwd2, gain, mine, theirs, inv4, w, early, acc) = refs[0:10]
    y, v, sums = refs[12:15]
    count = rows // SUB + 1
    sub = sublanes((SUB, cols + LANE))
    for slot, t in enumerate((count - 2, count - 1, 0, 1, *range(begin, count - 2))):
        middle = (mine[tile(slot), :] + theirs[tile(slot), :]) * inv4[tile(t), :]
        back(depth, t, fwd2, gain, middle, y)
    carry = (acc[0], acc[1])
    for t, n in ((begin - 1, count - begin), (0, 3)):
        carry = second_image_of(depth, cols, t, n, count, sub, (row, col, w, y, v), carry)
    sums[...] = gathered(sums, (early[0], early[1], *carry))


def final_kernel(depth, rows, cols, *refs):
    (sums, right, z, w, y, v, x_out, r_out, x, r, sem) = refs
    core, _, _ = position()
    total = jnp.sum(sums[...], axis=0, keepdims=True)
    lane = lanes(total.shape)
    rho, c, e, g = (
        jnp.sum(jnp.where(lane == i, total, 0.0), axis=1, keepdims=True) for i in range(4)
    )
    alpha = rho / c
    rho1 = alpha * (alpha * e - c)
    beta = rho1 / rho
    curvature = c - 2.0 * alpha * e + alpha * alpha * g
    alpha1 = rho1 / (curvature - beta * beta * c)
    near = jnp.broadcast_to(alpha + alpha1 * (1.0 + beta), (SUB, cols))
    far = jnp.broadcast_to(alpha1 * alpha, (SUB, cols))
    copies = []
    for k in range(depth):

        def body(t, carry, k=k):
            x[k, tile(t), :] = near * z[k, tile(t), 0:cols] - far * y[k, tile(t), 0:cols]
            r[k, tile(t), :] = (
                right[k, tile(t), 0:cols] - near * w[k, tile(t), 0:cols] + far * v[k, tile(t), :]
            )
            return carry

        sweep(0, rows // SUB, FINAL, each(body))
        at = layer_of(core, k, depth)
        for slot, (value, target) in enumerate(((x, x_out), (r, r_out))):
            copy = pltpu.make_async_copy(value.at[k], target.at[at], sem.at[slot, k])
            copy.start()
            copies.append(copy)
    for copy in copies:
        copy.wait()


def shift(value, axis, by):
    count = lax.axis_size(axis)
    return lax.ppermute(value, axis, [(i, (i + by) % count) for i in range(count)])


def shards(right_side, row_conduct, column_conduct, via_conduct, via_mask, ground_conduct):
    depth, rows, cols = right_side.shape
    places = (lax.axis_size(PX), lax.axis_size("py"))
    devices = lax.axis_size(ALL)
    tall, wide = rows + SUB, cols + LANE
    ext = (depth, tall, wide)
    vmem, hbm = pltpu.VMEM, pltpu.HBM
    size = depth * tall * wide
    part = functools.partial

    inputs = [right_side, row_conduct, column_conduct, via_conduct, ground_conduct, via_mask]
    strips = (FIELDS * depth * 2, LANE)
    *e, msg_right, msg_left = call(
        part(load_kernel, depth, rows, cols),
        inputs,
        [hbm] * 6,
        [ext] * FIELDS + [strips] * 2,
        [
            pltpu.VMEM((depth, rows, 2 * LANE), jnp.int32),
            pltpu.VMEM((2, rows, LANE), jnp.float32),
            pltpu.SemaphoreType.DMA((3, 6, depth)),
        ],
        flops=size,
        moved=6 * size,
    )
    from_left = shift(msg_right, "py", 1)
    from_right = shift(msg_left, "py", -1)
    e = call(
        part(middle_kernel, depth, rows, cols),
        [*inputs, *e],
        [hbm] * 6 + [vmem] * FIELDS,
        [ext] * FIELDS,
        [
            pltpu.VMEM((depth, rows, cols - 2 * LANE), jnp.int32),
            pltpu.SemaphoreType.DMA((1, 6, depth)),
        ],
        alias={6 + i: i for i in range(FIELDS)},
        flops=10 * size,
        moved=18 * size,
    )
    strips = (FIELDS * depth * 2, wide)
    *e, msg_down, msg_up, both = call(
        part(column_kernel, depth, rows, cols, places[1]),
        [*e, from_left, from_right],
        [vmem] * 7,
        [ext] * FIELDS + [strips] * 2 + [(rows, LANE)],
        alias={i: i for i in range(FIELDS)},
        flops=size,
    )
    from_above = shift(msg_down, PX, 1)
    from_below = shift(msg_up, PX, -1)
    end = rows // SUB
    split = end // 2 + 1
    flops = 15 * size
    *state, mine = call(
        part(inner_kernel, depth, rows, cols, places, 1, split, 0),
        [*e, both],
        [vmem] * 6,
        [ext] * FIELDS + [ext] * 3 + [(2, (split - 1) * SUB, wide)],
        alias={i: i for i in range(FIELDS)},
        flops=flops,
    )
    theirs = shift(mine, "layer", 1)
    *state, mine_rest = call(
        part(inner_kernel, depth, rows, cols, places, split, end, 3),
        [*state, both],
        [vmem] * 9,
        [ext] * FIELDS + [ext] * 3 + [(2, (end - split) * SUB, wide)],
        alias={i: i for i in range(FIELDS + 3)},
        flops=flops,
    )
    theirs_rest = shift(mine_rest, "layer", 1)
    right, row, col, via, _, fwd, gain, inv = state
    late = end - 1 - TAIL
    images = [ext, (tall, wide), ext, ext, ((late - 2) * SUB, wide)]
    first = call(
        part(inner_image_kernel, depth, rows, cols, 1, split, 2, split - 1),
        [right, row, col, via, fwd, gain, inv, mine, theirs],
        [vmem] * 9,
        images,
        flops=flops,
    )
    z, inv4, w, fwd2, mine2 = call(
        part(inner_image_kernel, depth, rows, cols, split, end, split - 1, late),
        [right, row, col, via, fwd, gain, inv, mine_rest, theirs_rest, *first],
        [vmem] * 14,
        images,
        alias={9 + i: i for i in range(5)},
        flops=flops,
    )
    *e, fwd, gain, inv, mine_outer = call(
        part(outer_kernel, depth, rows, cols, places),
        [*state, from_above, from_below],
        [vmem] * 10,
        [ext] * FIELDS + [ext] * 3 + [(2, 2 * SUB, wide)],
        alias={i: i for i in range(FIELDS + 3)},
        flops=3 * size,
    )
    right, row, col, via, _ = e
    theirs_outer = shift(mine_outer, "layer", 1)
    theirs2 = shift(mine2, "layer", 1)
    w, fwd2, mine2_outer, early = call(
        part(tail_kernel, depth, rows, cols, late),
        [right, row, col, via, gain, inv, z, w, fwd2],
        [vmem] * 9,
        [ext, ext, ((4 + TAIL) * SUB, wide), (2, SUB, cols)],
        alias={7: 0, 8: 1},
        flops=8 * size,
    )
    z, inv4, w, fwd2, mine2_outer, early = call(
        part(outer_image_kernel, depth, rows, cols),
        [right, row, col, via, fwd, gain, inv, mine_outer, theirs_outer, early]
        + [z, inv4, w, fwd2, mine2_outer],
        [vmem] * 15,
        [ext, (tall, wide), ext, ext, ((4 + TAIL) * SUB, wide), (2, SUB, cols)],
        alias={10: 0, 11: 1, 12: 2, 13: 3, 14: 4},
        flops=8 * size,
    )
    theirs2_outer = shift(mine2_outer, "layer", 1)
    block = (depth, rows, cols)
    y, v, acc = call(
        part(inner_dots_kernel, depth, rows, cols, late),
        [row, col, fwd2, gain, mine2, theirs2, inv4, w],
        [vmem] * 8,
        [ext, block, (2, SUB, cols)],
        flops=20 * size,
    )
    y, v, sums = call(
        part(outer_dots_kernel, depth, rows, cols, late),
        [row, col, fwd2, gain, mine2_outer, theirs2_outer, inv4, w, early, acc, y, v],
        [vmem] * 12,
        [ext, block, (devices, LANE)],
        alias={10: 0, 11: 1},
        flops=8 * size,
    )
    sums = lax.all_to_all(sums.reshape(devices, 1, LANE), ALL, 0, 0).reshape(devices, LANE)
    result = jax.ShapeDtypeStruct(block, jnp.float32)
    return call(
        part(final_kernel, depth, rows, cols),
        [sums, right, z, w, y, v],
        [vmem] * 6,
        [result] * 2,
        [
            pltpu.VMEM((depth, rows, cols), jnp.float32),
            pltpu.VMEM((depth, rows, cols), jnp.float32),
            pltpu.SemaphoreType.DMA((2, depth)),
        ],
        flops=10 * size,
    )


def solution(mesh):
    count = mesh.shape["px"]
    inner = 4 if count % 4 == 0 else 1
    split = Mesh(
        mesh.devices.reshape(mesh.shape["layer"], count // inner, inner, mesh.shape["py"]),
        ALL,
    )
    spec = P("layer", PX, "py")

    def step(*arrays):
        return tuple(shards(*arrays))

    return jax.shard_map(
        step,
        mesh=split,
        in_specs=(spec,) * 6,
        out_specs=(spec, spec),
        check_vma=False,
    )
```
